8 devices in a mesh: dp: 1 (over z), seq: 8 (over y, x, core).
Axes of the slice: x: 2, y: 2, z: 1, core: 2. Of those that a mesh axis runs over, the one named last changes fastest.
Arguments:
- enc_out: bfloat16 [64, 16, 640], P('dp', 'seq')
- pred_out: bfloat16 [64, 8, 640], P('dp')
- w_enc: bfloat16 [640, 640], replicated
- w_pred: bfloat16 [640, 640], replicated
- w_out: bfloat16 [640, 4096], replicated
- labels: int32 [64, 7], P('dp')
- frame_len: int32 [64], P('dp')
- label_len: int32 [64], P('dp')
Outputs:
- output 1: float32 [64], P('dp')
- output 2: bfloat16 [64, 16, 640], P('dp', 'seq')
- output 3: float32 [640, 640], P('dp')
- output 4: float32 [640, 640], P('dp')
- output 5: float32 [640, 4096], P('dp')
All inputs are finite; a program needn't handle non-finite values.
Results may differ from the reference program's by a relative error of at most 0.0134743.
Values are sent between devices in bfloat16 or wider.
A program may use at most 1 GiB of HBM per device.

```python
import jax
import jax.numpy as jnp
from jax import lax

NUM_UTT = 64
NUM_FRAMES = 16
LABEL_POS = 8
ENC_DIM = 640
PRED_DIM = 640
JOINT_DIM = 640
VOCAB_SIZE = 4096
FRAME_BLOCK = 2
NUM_LABELS = LABEL_POS - 1
NUM_BLOCKS = NUM_FRAMES // FRAME_BLOCK
NEG_FILL = -1.0e30


def setup_inputs(seed: int = 0, part: int = 0) -> dict:
    shared_key, part_base = jax.random.split(jax.random.key(seed))
    part_key = jax.random.fold_in(part_base, part)
    k_enc, k_pred, k_lab, k_frames, k_lens = jax.random.split(part_key, 5)
    k_wenc, k_wpred, k_wout = jax.random.split(shared_key, 3)
    enc_out = jax.random.normal(k_enc, (NUM_UTT, NUM_FRAMES, ENC_DIM), jnp.float32).astype(jnp.bfloat16)
    pred_out = jax.random.normal(k_pred, (NUM_UTT, LABEL_POS, PRED_DIM), jnp.float32).astype(jnp.bfloat16)
    w_enc = (jax.random.normal(k_wenc, (ENC_DIM, JOINT_DIM), jnp.float32) * ENC_DIM ** -0.5).astype(jnp.bfloat16)
    w_pred = (jax.random.normal(k_wpred, (PRED_DIM, JOINT_DIM), jnp.float32) * PRED_DIM ** -0.5).astype(jnp.bfloat16)
    w_out = (jax.random.normal(k_wout, (JOINT_DIM, VOCAB_SIZE), jnp.float32) * (1.5 * JOINT_DIM ** -0.5)).astype(jnp.bfloat16)
    labels = jax.random.randint(k_lab, (NUM_UTT, NUM_LABELS), 1, VOCAB_SIZE, jnp.int32)
    frame_len = jax.random.randint(k_frames, (NUM_UTT,), NUM_FRAMES // 4 + 1, NUM_FRAMES + 1, jnp.int32).at[0].set(NUM_FRAMES)
    label_len = jax.random.randint(k_lens, (NUM_UTT,), 1, NUM_LABELS + 1, jnp.int32).at[NUM_UTT - 1].set(NUM_LABELS)
    return {'enc_out': enc_out, 'pred_out': pred_out, 'w_enc': w_enc, 'w_pred': w_pred, 'w_out': w_out, 'labels': labels, 'frame_len': frame_len, 'label_len': label_len}


def joint_block(enc_blk, act_g, w_enc, w_out):
    n_utt, n_blk, _ = enc_blk.shape
    act_f = jnp.dot(enc_blk.reshape(n_utt * n_blk, ENC_DIM), w_enc, preferred_element_type=jnp.float32).astype(jnp.bfloat16).reshape(n_utt, n_blk, JOINT_DIM)
    hidden = jnp.tanh(act_f[:, :, None, :].astype(jnp.float32) + act_g[:, None, :, :].astype(jnp.float32)).astype(jnp.bfloat16)
    logits = jnp.dot(hidden.reshape(n_utt * n_blk * LABEL_POS, JOINT_DIM), w_out, preferred_element_type=jnp.float32).reshape(n_utt, n_blk, LABEL_POS, VOCAB_SIZE)
    return hidden, jax.nn.log_softmax(logits, axis=-1)


def label_prefix(frame_lab):
    zero_col = jnp.zeros_like(frame_lab[:, :1])
    return jnp.concatenate([zero_col, jnp.cumsum(frame_lab, axis=1)], axis=1)


def reference(enc_out, pred_out, w_enc, w_pred, w_out, labels, frame_len, label_len):
    act_g = jnp.dot(pred_out.reshape(NUM_UTT * LABEL_POS, PRED_DIM), w_pred, preferred_element_type=jnp.float32).astype(jnp.bfloat16).reshape(NUM_UTT, LABEL_POS, JOINT_DIM)
    lab_ids = jnp.concatenate([labels, jnp.full((NUM_UTT, 1), -1, jnp.int32)], axis=1)
    lab_index = jnp.broadcast_to(labels[:, None, :, None], (NUM_UTT, FRAME_BLOCK, NUM_LABELS, 1))
    enc_blocks = enc_out.reshape(NUM_UTT, NUM_BLOCKS, FRAME_BLOCK, ENC_DIM).transpose(1, 0, 2, 3)

    def lattice_scores(enc_blk):
        _, log_probs = joint_block(enc_blk, act_g, w_enc, w_out)
        lab_lp = jnp.take_along_axis(log_probs[:, :, :NUM_LABELS, :], lab_index, axis=3)[..., 0]
        return log_probs[..., 0], lab_lp

    blank_blocks, lab_blocks = lax.map(lattice_scores, enc_blocks)
    blank_lp = blank_blocks.transpose(1, 0, 2, 3).reshape(NUM_UTT, NUM_FRAMES, LABEL_POS)
    lab_lp = lab_blocks.transpose(1, 0, 2, 3).reshape(NUM_UTT, NUM_FRAMES, NUM_LABELS)

    pos_ids = jnp.arange(LABEL_POS)[None, :]
    neg_rows = jnp.full((NUM_UTT, LABEL_POS), NEG_FILL, jnp.float32)
    init_x = jnp.where(pos_ids == 0, 0.0, neg_rows)
    boundary = jnp.where(pos_ids == label_len[:, None], 0.0, neg_rows)

    def alpha_step(x_prev, frame_in):
        frame_blank, frame_lab = frame_in
        lab_sum = label_prefix(frame_lab)
        alpha_t = lab_sum + lax.cumlogsumexp(x_prev - lab_sum, axis=1)
        return alpha_t + frame_blank, alpha_t

    _, alphas = lax.scan(alpha_step, init_x, (blank_lp.transpose(1, 0, 2), lab_lp.transpose(1, 0, 2)))
    alphas = alphas.transpose(1, 0, 2)

    def beta_step(next_row, frame_in):
        frame_blank, frame_lab, frame_id = frame_in
        lab_sum = label_prefix(frame_lab)
        beta_row = lax.cumlogsumexp(next_row + frame_blank + lab_sum, axis=1, reverse=True) - lab_sum
        beta_row = jnp.where((frame_id >= frame_len)[:, None], boundary, beta_row)
        return beta_row, (beta_row, next_row)

    first_row, (betas, beta_next) = lax.scan(beta_step, boundary, (blank_lp.transpose(1, 0, 2), lab_lp.transpose(1, 0, 2), jnp.arange(NUM_FRAMES)), reverse=True)
    betas = betas.transpose(1, 0, 2)
    beta_next = beta_next.transpose(1, 0, 2)
    log_prob = first_row[:, 0]

    beta_up = jnp.concatenate([betas[:, :, 1:], jnp.full((NUM_UTT, NUM_FRAMES, 1), NEG_FILL, jnp.float32)], axis=2)
    lab_full = jnp.concatenate([lab_lp, jnp.zeros((NUM_UTT, NUM_FRAMES, 1), jnp.float32)], axis=2)
    frame_ok = (jnp.arange(NUM_FRAMES)[None, :] < frame_len[:, None])[:, :, None]
    norm_shift = log_prob[:, None, None]
    occ_blank = jnp.where(frame_ok, jnp.exp(jnp.minimum(alphas + blank_lp + beta_next - norm_shift, 0.0)), 0.0)
    occ_lab = jnp.where(frame_ok, jnp.exp(jnp.minimum(alphas + lab_full + beta_up - norm_shift, 0.0)), 0.0)

    def to_blocks(arr):
        return arr.reshape(NUM_UTT, NUM_BLOCKS, FRAME_BLOCK, LABEL_POS).transpose(1, 0, 2, 3)

    vocab_ids = jnp.arange(VOCAB_SIZE)

    def grad_step(acc_carry, blk_in):
        gw_enc, gw_out, d_act_g = acc_carry
        enc_blk, occ_b, occ_l = blk_in
        hidden, log_probs = joint_block(enc_blk, act_g, w_enc, w_out)
        d_logits = (jnp.exp(log_probs) * (occ_b + occ_l)[..., None] - jnp.where(vocab_ids == 0, occ_b[..., None], 0.0) - jnp.where(vocab_ids == lab_ids[:, None, :, None], occ_l[..., None], 0.0)).astype(jnp.bfloat16)
        flat_dz = d_logits.reshape(NUM_UTT * FRAME_BLOCK * LABEL_POS, VOCAB_SIZE)
        flat_h = hidden.reshape(NUM_UTT * FRAME_BLOCK * LABEL_POS, JOINT_DIM)
        d_hidden = jnp.dot(flat_dz, w_out.T, preferred_element_type=jnp.float32)
        d_pre = (d_hidden * (1.0 - jnp.square(flat_h.astype(jnp.float32)))).astype(jnp.bfloat16).reshape(NUM_UTT, FRAME_BLOCK, LABEL_POS, JOINT_DIM)
        d_act_f = jnp.sum(d_pre.astype(jnp.float32), axis=2).astype(jnp.bfloat16).reshape(NUM_UTT * FRAME_BLOCK, JOINT_DIM)
        grad_blk = jnp.dot(d_act_f, w_enc.T, preferred_element_type=jnp.float32).astype(jnp.bfloat16).reshape(NUM_UTT, FRAME_BLOCK, ENC_DIM)
        gw_enc = gw_enc + jnp.dot(enc_blk.reshape(NUM_UTT * FRAME_BLOCK, ENC_DIM).T, d_act_f, preferred_element_type=jnp.float32)
        gw_out = gw_out + jnp.dot(flat_h.T, flat_dz, preferred_element_type=jnp.float32)
        d_act_g = d_act_g + jnp.sum(d_pre.astype(jnp.float32), axis=1)
        return (gw_enc, gw_out, d_act_g), grad_blk

    acc_init = (jnp.zeros((ENC_DIM, JOINT_DIM), jnp.float32), jnp.zeros((JOINT_DIM, VOCAB_SIZE), jnp.float32), jnp.zeros((NUM_UTT, LABEL_POS, JOINT_DIM), jnp.float32))
    (gw_enc, gw_out, d_act_g), grad_blocks = lax.scan(grad_step, acc_init, (enc_blocks, to_blocks(occ_blank), to_blocks(occ_lab)))
    grad_enc = grad_blocks.transpose(1, 0, 2, 3).reshape(NUM_UTT, NUM_FRAMES, ENC_DIM)
    gw_pred = jnp.einsum('buh,buj->hj', pred_out.astype(jnp.float32), d_act_g.astype(jnp.float32))
    return -log_prob, grad_enc, gw_enc, gw_pred, gw_out
```

```python
import jax
import jax.numpy as jnp
from jax import lax
from jax.experimental import pallas as pl
from jax.experimental.pallas import tpu as pltpu
from jax.sharding import PartitionSpec as P

NEG = -1.0e30
F32 = jnp.float32
BF16 = jnp.bfloat16
N_DEV = 8
DIM = 640
VOCAB = 4096
LANES = 1024
CHUNK = 256
VMEM_LIMIT = 66_000_000


def dot_nn(lhs, rhs):
    return lax.dot_general(lhs, rhs, (((1,), (0,)), ((), ())), preferred_element_type=F32)


def dot_nt(lhs, rhs):
    return lax.dot_general(lhs, rhs, (((1,), (1,)), ((), ())), preferred_element_type=F32)


def iota(shape, axis):
    return lax.broadcasted_iota(jnp.int32, shape, axis)


def eye(size):
    return jnp.where(iota((size, size), 0) == iota((size, size), 1), 1.0, 0.0).astype(BF16)


def transpose_into(dst, src, ident):
    cols = src.shape[1]
    for lo in range(0, cols, 256):
        width = min(256, cols - lo)
        dst[lo:lo + width, :] = dot_nt(ident[:width, :width], src[:, lo:lo + width]).astype(BF16)


def logaddexp(a, b):
    top = jnp.maximum(a, b)
    return top + jnp.log(1.0 + jnp.exp(-jnp.abs(a - b)))


class Peers:
    def __init__(self):
        self.dp = lax.axis_index('dp')
        self.me = lax.axis_index('seq')
        core = lax.rem(self.me, 2)
        col = lax.rem(self.me // 2, 2)
        row = self.me // 4
        self.pp = row * 4 + col * 2 + (1 - core)
        self.px = row * 4 + (1 - col) * 2 + core
        self.py = (1 - row) * 4 + col * 2 + core
        self.pd = (1 - row) * 4 + (1 - col) * 2 + core
        self.px_p = row * 4 + (1 - col) * 2 + (1 - core)
        self.py_p = (1 - row) * 4 + col * 2 + (1 - core)
        self.pd_p = (1 - row) * 4 + (1 - col) * 2 + (1 - core)

    def target(self, seq):
        return (self.dp, seq)


def remote(src, dst, send_sem, recv_sem, device):
    return pltpu.make_async_remote_copy(src_ref=src, dst_ref=dst, send_sem=send_sem, recv_sem=recv_sem,
                                        device_id=device, device_id_type=pl.DeviceIdType.MESH)


class Relay:
    def __init__(self, peers, view, half, send_sem, recv_sem):
        self.p = peers
        self.view = view
        self.half = half
        self.ssem = send_sem
        self.rsem = recv_sem

    def copy(self, kind, block, device):
        return remote(block, block, self.ssem.at[kind], self.rsem.at[kind], self.p.target(device))

    def start(self):
        p = self.p
        for kind, dev in ((1, p.px), (2, p.py), (0, p.pp)):
            self.copy(kind, self.view(p.me), dev).start()

    def pass_on(self):
        p = self.p
        self.copy(1, self.view(p.px), p.px).wait_recv()
        self.copy(4, self.half(p.px, 0), p.py).start()
        self.copy(3, self.view(p.px), p.pp).start()
        self.copy(2, self.view(p.py), p.py).wait_recv()
        self.copy(6, self.half(p.py, 1), p.px).start()
        self.copy(5, self.view(p.py), p.pp).start()

    def pass_diagonal(self):
        p = self.p
        self.copy(4, self.half(p.pd, 0), p.py).wait_recv()
        self.copy(7, self.half(p.pd, 0), p.pp).start()
        self.copy(6, self.half(p.pd, 1), p.px).wait_recv()
        self.copy(8, self.half(p.pd, 1), p.pp).start()

    def finish(self):
        p = self.p
        self.copy(0, self.view(p.pp), p.pp).wait_recv()
        self.copy(3, self.view(p.px_p), p.pp).wait_recv()
        self.copy(5, self.view(p.py_p), p.pp).wait_recv()
        self.copy(7, self.half(p.pd_p, 0), p.pp).wait_recv()
        self.copy(8, self.half(p.pd_p, 1), p.pp).wait_recv()
        self.copy(0, self.view(p.me), p.pp).wait_send()
        self.copy(1, self.view(p.me), p.px).wait_send()
        self.copy(2, self.view(p.me), p.py).wait_send()
        self.copy(3, self.view(p.px), p.pp).wait_send()
        self.copy(4, self.half(p.px, 0), p.py).wait_send()
        self.copy(5, self.view(p.py), p.pp).wait_send()
        self.copy(6, self.half(p.py, 1), p.px).wait_send()
        self.copy(7, self.half(p.pd, 0), p.pp).wait_send()
        self.copy(8, self.half(p.pd, 1), p.pp).wait_send()


class Direct:
    def __init__(self, peers, src, dst, send_sem, recv_sem):
        self.p = peers
        self.src = src
        self.dst = dst
        self.ssem = send_sem
        self.rsem = recv_sem

    def copy(self, k, to, source):
        return remote(self.src(to), self.dst(source), self.ssem.at[k], self.rsem.at[k], self.p.target(to))

    def start(self):
        for k in range(1, N_DEV):
            self.copy(k, lax.rem(self.p.me + k, N_DEV), self.p.me).start()

    def wait_recv(self):
        for k in range(1, N_DEV):
            self.copy(k, lax.rem(self.p.me + k, N_DEV), lax.rem(self.p.me + N_DEV - k, N_DEV)).wait_recv()

    def wait_send(self):
        for k in range(1, N_DEV):
            self.copy(k, lax.rem(self.p.me + k, N_DEV), self.p.me).wait_send()


def pick_rows(ref, offsets, group):
    out = None
    for u, off in enumerate(offsets):
        part = ref[off:off + 24, :]
        out = part if out is None else jnp.where(group == u, part, out)
    return out


def lattice(lse, z_blank, z_lab, aux, me, skew, stats):
    lane = iota((1, 128), 1)
    group = lax.rem(lane // 8, 8)
    n_frames = aux[1, pl.ds(me, 1), :]
    n_labels = aux[2, pl.ds(me, 1), :]

    def by_time(x):
        return jnp.concatenate([x, pltpu.roll(x, 64, 1)], axis=0)

    skew[...] = jnp.zeros_like(skew)
    skew[0, 8:24, :] = by_time(z_blank - lse)
    skew[1, 8:24, :] = by_time(z_lab - lse)
    offsets = [8 - u for u in range(8)]
    group24 = jnp.broadcast_to(group, (24, 128))
    blank = pick_rows(skew.at[0], offsets, group24)
    lab = pick_rows(skew.at[1], offsets, group24)

    first_u = group == 0
    last_u = group == 7
    alpha = jnp.where(first_u, 0.0, NEG).astype(F32)
    alphas = [alpha]
    for d in range(1, 23):
        stay = alpha + blank[d - 1:d]
        step = jnp.where(first_u, NEG, pltpu.roll(alpha + lab[d - 1:d], 8, 1))
        alpha = logaddexp(stay, step)
        alphas.append(alpha)
    alphas.append(jnp.full((1, 128), NEG, F32))
    bound = jnp.where(group == n_labels, 0.0, NEG).astype(F32)
    beta = bound
    nexts, ups = [None] * 24, [None] * 24
    nexts[23] = ups[23] = jnp.full((1, 128), NEG, F32)
    for d in range(22, -1, -1):
        up = jnp.where(last_u, NEG, pltpu.roll(beta, 120, 1))
        nexts[d], ups[d] = beta, up
        new = logaddexp(beta + blank[d:d + 1], up + lab[d:d + 1])
        beta = jnp.where(d - group >= n_frames, bound, new)
    log_p = jnp.where(lane < 8, beta, 0.0)
    for shift in (8, 16, 32, 64):
        log_p = log_p + pltpu.roll(log_p, shift, 1)

    alphas = jnp.concatenate(alphas, axis=0)
    nexts = jnp.concatenate(nexts, axis=0)
    ups = jnp.concatenate(ups, axis=0)
    frame = iota((24, 128), 0) - group24
    ok = (frame >= 0) & (frame < n_frames)
    occ_b = jnp.where(ok, jnp.exp(jnp.minimum(alphas + blank + nexts - log_p, 0.0)), 0.0)
    occ_l = jnp.where(ok & (group24 < 7), jnp.exp(jnp.minimum(alphas + lab + ups - log_p, 0.0)), 0.0)
    skew[0, 0:24, :] = occ_b
    skew[1, 0:24, :] = occ_l
    offsets = list(range(8))
    low = jnp.broadcast_to(lane < 64, (8, 128))

    def by_tile(x):
        return jnp.where(low, x[0:8], pltpu.roll(x[8:16], 64, 1))

    stats[me, 0:8, :] = lse
    stats[me, 8:16, :] = by_tile(pick_rows(skew.at[0], offsets, group24))
    stats[me, 16:24, :] = by_tile(pick_rows(skew.at[1], offsets, group24))
    stats[me, 24:32, :] = jnp.broadcast_to(log_p, (8, 128))


def grad_logits(z, stats, block, lab, first_id, col0=0, has_blank=None):
    rows, cols = z.shape
    ids = iota((rows, 128), 0) + first_id
    tiles = []
    for k in range(cols // 128):
        kk = k + col0
        lse = stats[block, kk:kk + 1, :]
        occ_b = stats[block, 8 + kk:9 + kk, :]
        occ_l = stats[block, 16 + kk:17 + kk, :]
        tile = jnp.exp(z[:, k * 128:(k + 1) * 128] - lse) * (occ_b + occ_l)
        tile = tile - jnp.where(ids == lab, occ_l, 0.0)
        head = tile[0:16] - jnp.where(ids[0:16] == 0, occ_b, 0.0)
        tiles.append(jnp.concatenate([head, tile[16:]], axis=0).astype(BF16))
    return jnp.concatenate(tiles, axis=1)


def main_kernel(enc, g, w_enc, w_pred, w_out, aux,
                gw_buf, da_all, dc_all, f_all, stats,
                wt, ht, sel, act, wet, wpt, dh, skew, a2a_s, a2a_r, f_s, f_r, st_s, st_r,
                gw_s, gw_r, da_s, da_r, dc_s, dc_r):
    p = Peers()
    me = p.me
    barrier = pltpu.get_barrier_semaphore()
    for k in range(1, N_DEV):
        pl.semaphore_signal(barrier, inc=1, device_id=p.target(lax.rem(me + k, N_DEV)),
                            device_id_type=pl.DeviceIdType.MESH)
    pl.semaphore_wait(barrier, N_DEV - 1)

    def rows16(i):
        return pl.ds(pl.multiple_of(i * 16, 16), 16)

    copies = []
    for k in range(1, N_DEV):
        to = lax.rem(me + k, N_DEV)
        copies.append(remote(enc.at[rows16(to), :], f_all.at[to, rows16(me), :], a2a_s.at[k], a2a_r.at[k], p.target(to)))
    for c in copies:
        c.start()
    f_all[me, rows16(me), :] = enc[rows16(me), :]

    ident = eye(256)
    transpose_into(wet, w_enc, ident)
    transpose_into(wpt, w_pred, ident)

    def transpose_out(c, _):
        lo = pl.multiple_of(c * CHUNK, CHUNK)
        wt[pl.ds(lo, CHUNK), :] = dot_nt(ident, w_out[:, pl.ds(lo, CHUNK)]).astype(BF16)
        return 0

    lax.fori_loop(0, VOCAB // CHUNK, transpose_out, 0)
    row = iota((192, LANES), 0)
    col = iota((192, LANES), 1)
    t_id = col // 128 + 8 * (lax.rem(col, 128) // 64)
    u_id = lax.rem(col // 8, 8)
    b_id = lax.rem(col, 8)
    a_row = 2 * (row // 16) + lax.rem(row, 2)
    a_b = lax.rem(row // 2, 8)
    c_row = row - 128
    hit = jnp.where(row < 128, jnp.where((a_row == t_id) & (a_b == b_id), 1.0, 0.0),
                    jnp.where((c_row // 8 == b_id) & (lax.rem(c_row, 8) == u_id), 1.0, 0.0))
    sel[...] = hit.astype(BF16)

    for d in range(N_DEV):
        act[d, :, 128:192] = dot_nt(wpt[...], g[d * 64:(d + 1) * 64, :]).astype(BF16)

    for k in range(1, N_DEV):
        src = lax.rem(me + N_DEV - k, N_DEV)
        remote(enc.at[rows16(me), :], f_all.at[me, rows16(src), :], a2a_s.at[k], a2a_r.at[k], p.target(src)).wait_recv()

    f_gather = Direct(p, lambda d: f_all.at[me], lambda i: f_all.at[i], f_s, f_r)
    f_gather.start()

    def hidden(d):
        act[d, :, 0:128] = dot_nt(wet[...], f_all[d]).astype(BF16)
        ht[d] = jnp.tanh(dot_nn(act[d], sel[...])).astype(BF16)

    hidden(me)
    lab_own = aux[0, pl.ds(me, 1), :]

    def tile8(x):
        return jnp.concatenate([x] * 8, axis=1)

    lab_row = tile8(lab_own)

    def forward(c, carry):
        top, total, z_lab = carry
        lo = pl.multiple_of(c * CHUNK, CHUNK)
        z = dot_nn(wt[pl.ds(lo, CHUNK), :], ht[me]).reshape(CHUNK // 8, 8, LANES)
        new = jnp.maximum(top, jnp.max(z, axis=0))
        total = total * jnp.exp(top - new) + jnp.sum(jnp.exp(z - new[None]), axis=0)
        ids = iota((CHUNK // 8, 8, LANES), 0) * 8 + iota((CHUNK // 8, 8, LANES), 1) + lo
        z_lab = z_lab + jnp.sum(jnp.where(ids == lab_row[None], z, 0.0), axis=0)
        return new, total, z_lab

    start = (jnp.full((8, LANES), NEG, F32), jnp.zeros((8, LANES), F32), jnp.zeros((8, LANES), F32))
    top, total, z_lab = lax.fori_loop(0, VOCAB // CHUNK, forward, start)
    peak = jnp.max(top, axis=0, keepdims=True)
    lse = peak + jnp.log(jnp.sum(total * jnp.exp(top - peak), axis=0, keepdims=True))
    z_lab = jnp.sum(z_lab, axis=0, keepdims=True)
    z_blank = dot_nn(wt[0:16, :], ht[me])[0:1]

    def tiles(x):
        return jnp.concatenate([x[:, k * 128:(k + 1) * 128] for k in range(8)], axis=0)

    lattice(tiles(lse), tiles(z_blank), tiles(z_lab), aux, me, skew, stats)
    st_gather = Direct(p, lambda d: stats.at[me], lambda i: stats.at[i], st_s, st_r)
    st_gather.start()

    f_gather.wait_recv()

    def hidden_other(k, _):
        hidden(lax.rem(me + k, N_DEV))
        return 0

    lax.fori_loop(1, N_DEV, hidden_other, 0)
    st_gather.wait_recv()

    relays = []
    for c in range(2):
        def view(e, c=c):
            return gw_buf.at[2 * e + c]

        def half(e, h, c=c):
            return gw_buf.at[2 * e + c, pl.ds(h * 320, 320), :]

        relay = Relay(p, view, half, gw_s.at[c], gw_r.at[c])
        relays.append(relay)
        first = pl.multiple_of(me * 512 + c * CHUNK, CHUNK)
        gw_buf[2 * me + c] = jnp.zeros((DIM, CHUNK), F32)

        def block(d, _, c=c, first=first):
            z = dot_nn(wt[pl.ds(first, CHUNK), :], ht[d])
            dz = grad_logits(z, stats, d, aux[0, pl.ds(d, 1), :], first)
            gw_buf[2 * me + c] += dot_nt(ht[d], dz)
            return 0

        lax.fori_loop(0, N_DEV, block, 0)
        relay.start()

    dh[...] = jnp.zeros_like(dh)

    def backward(c, _):
        lo = pl.multiple_of(c * 512, 512)
        z = dot_nn(wt[pl.ds(lo, 512), :], ht[me])
        dz = grad_logits(z, stats, me, lab_own, lo)
        dh[...] += dot_nn(w_out[:, pl.ds(lo, 512)], dz)
        return 0

    lax.fori_loop(0, VOCAB // 512, backward, 0)
    relays[0].pass_on()
    h32 = ht[me].astype(F32)
    dp = (dh[...] * (1.0 - h32 * h32)).astype(BF16)
    sums = dot_nt(dp, sel[...])
    da_all[me] = sums[:, 0:128].astype(BF16)
    dc_all[me] = jnp.concatenate([sums[0:320, 128:192], sums[320:640, 128:192]], axis=1)
    da_relay = Relay(p, lambda e: da_all.at[e], lambda e, h: da_all.at[e, pl.ds(h * 320, 320), :], da_s, da_r)
    dc_relay = Relay(p, lambda e: dc_all.at[e], lambda e, h: dc_all.at[e, pl.ds(h * 160, 160), :], dc_s, dc_r)
    da_relay.start()
    dc_relay.start()
    relays[1].pass_on()
    da_relay.pass_on()
    dc_relay.pass_on()
    for relay in (relays[0], relays[1], da_relay, dc_relay):
        relay.pass_diagonal()
    for relay in (relays[0], relays[1], da_relay, dc_relay):
        relay.finish()
    for c in copies:
        c.wait_send()
    f_gather.wait_send()
    st_gather.wait_send()


def final_kernel(gw_buf, da_all, dc_all, f_all, g, w_enc, gw_out, grad_enc, gw_enc, gw_pred, ft, gt, out_sem):
    me = lax.axis_index('seq')
    flush = []
    for n in range(VOCAB // CHUNK):
        flush.append(pltpu.make_async_copy(gw_buf.at[n], gw_out.at[:, n * CHUNK:(n + 1) * CHUNK], out_sem.at[n]))
        flush[-1].start()
    ident = eye(256)
    for d in range(N_DEV):
        for lo in range(0, DIM, 256):
            width = min(256, DIM - lo)
            ft[lo:lo + width, d * 128:(d + 1) * 128] = dot_nt(ident[:width, :width], f_all[d, :, lo:lo + width]).astype(BF16)
    transpose_into(gt, g, ident)
    da = jnp.concatenate([da_all[d] for d in range(N_DEV)], axis=1)
    gw_enc[...] = dot_nt(ft[...], da)
    pick = jnp.where(iota((16, 128), 1) == iota((16, 128), 0) + me * 16, 1.0, 0.0).astype(BF16)
    mine = jnp.concatenate([dot_nt(pick, da_all[d]).astype(BF16) for d in range(N_DEV)], axis=0)
    grad_enc[...] = dot_nt(mine, w_enc[...]).astype(BF16)
    dc = jnp.concatenate([jnp.concatenate([dc_all[d, :, 0:64], dc_all[d, :, 64:128]], axis=0) for d in range(N_DEV)], axis=1)
    gw_pred[...] = dot_nt(gt[...], dc.astype(BF16))
    for copy in flush:
        copy.wait()


def vmem():
    return pl.BlockSpec(memory_space=pltpu.VMEM)


def solution(mesh):
    dma = pltpu.SemaphoreType.DMA

    def local_fn(enc_out, pred_out, w_enc, w_pred, w_out, labels, frame_len, label_len):
        n_utt = pred_out.shape[0]
        enc = enc_out.reshape(2 * n_utt, DIM)
        g = pred_out.reshape(8 * n_utt, DIM)
        lab = jnp.concatenate([labels, jnp.full((n_utt, 1), -1, jnp.int32)], axis=1)
        lab = lab.reshape(8, 8, 8).transpose(0, 2, 1)
        lens = jnp.broadcast_to(jnp.stack([frame_len, label_len]).reshape(2, 8, 1, 8), (2, 8, 8, 8))
        aux = jnp.concatenate([lab[None], lens], axis=0).reshape(3, 8, 64)
        aux = jnp.concatenate([aux, aux], axis=2)
        gw_buf, da_all, dc_all, f_all, stats = pl.pallas_call(
            main_kernel,
            out_shape=(jax.ShapeDtypeStruct((16, DIM, CHUNK), F32),
                       jax.ShapeDtypeStruct((8, DIM, 128), BF16),
                       jax.ShapeDtypeStruct((8, DIM // 2, 128), F32),
                       jax.ShapeDtypeStruct((8, 128, DIM), BF16),
                       jax.ShapeDtypeStruct((8, 32, 128), F32)),
            in_specs=[vmem()] * 6,
            out_specs=(vmem(),) * 5,
            scratch_shapes=[pltpu.VMEM((VOCAB, DIM), BF16), pltpu.VMEM((8, DIM, LANES), BF16),
                            pltpu.VMEM((192, LANES), BF16), pltpu.VMEM((8, DIM, 192), BF16),
                            pltpu.VMEM((DIM, DIM), BF16), pltpu.VMEM((DIM, DIM), BF16),
                            pltpu.VMEM((DIM, LANES), F32), pltpu.VMEM((2, 40, 128), F32),
                            dma((8,)), dma((8,)), dma((8,)), dma((8,)), dma((8,)), dma((8,)),
                            dma((2, 9)), dma((2, 9)), dma((9,)), dma((9,)), dma((9,)), dma((9,))],
            compiler_params=pltpu.CompilerParams(collective_id=0, has_side_effects=True, vmem_limit_bytes=VMEM_LIMIT),
        )(enc, g, w_enc, w_pred, w_out, aux)
        gw_out, grad_enc, gw_enc, gw_pred = pl.pallas_call(
            final_kernel,
            out_shape=(jax.ShapeDtypeStruct((DIM, VOCAB), F32),
                       jax.ShapeDtypeStruct((2 * n_utt, DIM), BF16),
                       jax.ShapeDtypeStruct((DIM, DIM), F32),
                       jax.ShapeDtypeStruct((DIM, DIM), F32)),
            in_specs=[vmem()] * 6,
            out_specs=(pl.BlockSpec(memory_space=pl.ANY), vmem(), vmem(), vmem()),
            scratch_shapes=[pltpu.VMEM((DIM, LANES), BF16), pltpu.VMEM((DIM, 512), BF16), dma((16,))],
            compiler_params=pltpu.CompilerParams(vmem_limit_bytes=VMEM_LIMIT),
        )(gw_buf, da_all, dc_all, f_all, g, w_enc)
        loss = -stats[:, 24, 0:8].reshape(n_utt)
        return loss, grad_enc.reshape(enc_out.shape), gw_enc, gw_pred, gw_out

    in_specs = (P('dp', 'seq', None), P('dp', None, None), P(None, None), P(None, None), P(None, None), P('dp', None), P('dp'), P('dp'))
    out_specs = (P('dp'), P('dp', 'seq', None), P('dp', None), P('dp', None), P('dp', None))
    return jax.shard_map(local_fn, mesh=mesh, in_specs=in_specs, out_specs=out_specs, check_vma=False)
```

```python
import jax
import jax.numpy as jnp
from jax import lax
from jax.experimental import pallas as pl
from jax.experimental.pallas import tpu as pltpu
from jax.sharding import PartitionSpec as P

NEG = -1.0e30
F32 = jnp.float32
BF16 = jnp.bfloat16
N_DEV = 8
DIM = 640
VOCAB = 4096
LANES = 1024
CHUNK = 256
MAIN_VMEM = 48 << 20
LAST_VMEM = 20 << 20


def dot_nn(lhs, rhs):
    return lax.dot_general(lhs, rhs, (((1,), (0,)), ((), ())), preferred_element_type=F32)


def dot_nt(lhs, rhs):
    return lax.dot_general(lhs, rhs, (((1,), (1,)), ((), ())), preferred_element_type=F32)


def iota(shape, axis):
    return lax.broadcasted_iota(jnp.int32, shape, axis)


def eye(size):
    return jnp.where(iota((size, size), 0) == iota((size, size), 1), 1.0, 0.0).astype(BF16)


def transpose_into(dst, src, ident):
    cols = src.shape[1]
    for lo in range(0, cols, 256):
        width = min(256, cols - lo)
        dst[lo:lo + width, :] = dot_nt(ident[:width, :width], src[:, lo:lo + width]).astype(BF16)


def logaddexp(a, b):
    top = jnp.maximum(a, b)
    return top + jnp.log(1.0 + jnp.exp(-jnp.abs(a - b)))


class Peers:
    def __init__(self):
        self.dp = lax.axis_index('dp')
        self.me = lax.axis_index('seq')
        core = lax.rem(self.me, 2)
        col = lax.rem(self.me // 2, 2)
        row = self.me // 4
        self.core = core
        self.diag = lax.rem(row + col, 2)
        self.pp = row * 4 + col * 2 + (1 - core)
        self.px = row * 4 + (1 - col) * 2 + core
        self.py = (1 - row) * 4 + col * 2 + core
        self.pd = (1 - row) * 4 + (1 - col) * 2 + core
        self.px_p = row * 4 + (1 - col) * 2 + (1 - core)
        self.py_p = (1 - row) * 4 + col * 2 + (1 - core)
        self.pd_p = (1 - row) * 4 + (1 - col) * 2 + (1 - core)

    def target(self, seq):
        return (self.dp, seq)


def remote(src, dst, send_sem, recv_sem, device):
    return pltpu.make_async_remote_copy(src_ref=src, dst_ref=dst, send_sem=send_sem, recv_sem=recv_sem,
                                        device_id=device, device_id_type=pl.DeviceIdType.MESH)


class Relay:
    def __init__(self, peers, view, half, send_sem, recv_sem):
        self.p = peers
        self.view = view
        self.half = half
        self.ssem = send_sem
        self.rsem = recv_sem

    def copy(self, kind, block, device):
        return remote(block, block, self.ssem.at[kind], self.rsem.at[kind], self.p.target(device))

    def start(self):
        p = self.p
        for kind, dev in ((1, p.px), (2, p.py), (0, p.pp)):
            self.copy(kind, self.view(p.me), dev).start()

    def pass_on(self):
        p = self.p
        self.copy(1, self.view(p.px), p.px).wait_recv()
        self.copy(4, self.half(p.px, 0), p.py).start()
        self.copy(3, self.view(p.px), p.pp).start()
        self.copy(2, self.view(p.py), p.py).wait_recv()
        self.copy(6, self.half(p.py, 1), p.px).start()
        self.copy(5, self.view(p.py), p.pp).start()

    def pass_diagonal(self):
        p = self.p
        self.copy(4, self.half(p.pd, 0), p.py).wait_recv()
        self.copy(7, self.half(p.pd, 0), p.pp).start()
        self.copy(6, self.half(p.pd, 1), p.px).wait_recv()
        self.copy(8, self.half(p.pd, 1), p.pp).start()

    def finish(self):
        p = self.p
        self.copy(0, self.view(p.pp), p.pp).wait_recv()
        self.copy(3, self.view(p.px_p), p.pp).wait_recv()
        self.copy(5, self.view(p.py_p), p.pp).wait_recv()
        self.copy(7, self.half(p.pd_p, 0), p.pp).wait_recv()
        self.copy(8, self.half(p.pd_p, 1), p.pp).wait_recv()
        self.copy(0, self.view(p.me), p.pp).wait_send()
        self.copy(1, self.view(p.me), p.px).wait_send()
        self.copy(2, self.view(p.me), p.py).wait_send()
        self.copy(3, self.view(p.px), p.pp).wait_send()
        self.copy(4, self.half(p.px, 0), p.py).wait_send()
        self.copy(5, self.view(p.py), p.pp).wait_send()
        self.copy(6, self.half(p.py, 1), p.px).wait_send()
        self.copy(7, self.half(p.pd, 0), p.pp).wait_send()
        self.copy(8, self.half(p.pd, 1), p.pp).wait_send()


class Pair:
    def __init__(self, peers, buf, mine, other, send_sem, recv_sem):
        self.p = peers
        self.buf = buf
        self.mine = mine
        self.other = other
        self.ssem = send_sem
        self.rsem = recv_sem

    def copy(self, c, kind, block, device):
        return remote(block, block, self.ssem.at[c, kind], self.rsem.at[c, kind], self.p.target(device))

    def half(self, base, core, c, h):
        return self.buf.at[(base + core) * 4 + c, h * 320:(h + 1) * 320, :]

    def start(self, c):
        p = self.p
        self.copy(c, 1, self.half(self.mine, p.core, c, 0), p.px).start()
        self.copy(c, 2, self.half(self.mine, p.core, c, 1), p.py).start()
        self.copy(c, 0, self.buf.at[(self.mine + p.core) * 4 + c], p.pp).start()

    def pass_on(self, c):
        p = self.p
        low = self.half(self.other, p.core, c, 0)
        high = self.half(self.other, p.core, c, 1)
        self.copy(c, 1, low, p.px).wait_recv()
        self.copy(c, 3, low, p.pp).start()
        self.copy(c, 2, high, p.py).wait_recv()
        self.copy(c, 4, high, p.pp).start()

    def finish(self, c):
        p = self.p
        twin = 1 - p.core
        self.copy(c, 0, self.buf.at[(self.mine + twin) * 4 + c], p.pp).wait_recv()
        self.copy(c, 3, self.half(self.other, twin, c, 0), p.pp).wait_recv()
        self.copy(c, 4, self.half(self.other, twin, c, 1), p.pp).wait_recv()
        self.copy(c, 0, self.buf.at[(self.mine + p.core) * 4 + c], p.pp).wait_send()
        self.copy(c, 1, self.half(self.mine, p.core, c, 0), p.px).wait_send()
        self.copy(c, 2, self.half(self.mine, p.core, c, 1), p.py).wait_send()
        self.copy(c, 3, self.half(self.other, p.core, c, 0), p.pp).wait_send()
        self.copy(c, 4, self.half(self.other, p.core, c, 1), p.pp).wait_send()


class Direct:
    def __init__(self, peers, src, dst, send_sem, recv_sem):
        self.p = peers
        self.src = src
        self.dst = dst
        self.ssem = send_sem
        self.rsem = recv_sem

    def copy(self, k, to, source):
        return remote(self.src(to), self.dst(source), self.ssem.at[k], self.rsem.at[k], self.p.target(to))

    def start(self):
        for k in range(1, N_DEV):
            self.copy(k, lax.rem(self.p.me + k, N_DEV), self.p.me).start()

    def wait_recv(self):
        for k in range(1, N_DEV):
            self.copy(k, lax.rem(self.p.me + k, N_DEV), lax.rem(self.p.me + N_DEV - k, N_DEV)).wait_recv()

    def wait_send(self):
        for k in range(1, N_DEV):
            self.copy(k, lax.rem(self.p.me + k, N_DEV), self.p.me).wait_send()


def pick_rows(ref, offsets, group):
    out = None
    for u, off in enumerate(offsets):
        part = ref[off:off + 24, :]
        out = part if out is None else jnp.where(group == u, part, out)
    return out


def lattice(lse, z_blank, z_lab, n_frames, n_labels, me, skew, stats):
    lane = iota((1, 128), 1)
    group = lax.rem(lane // 8, 8)

    def by_time(x):
        return jnp.concatenate([x, pltpu.roll(x, 64, 1)], axis=0)

    skew[...] = jnp.zeros_like(skew)
    skew[0, 8:24, :] = by_time(z_blank - lse)
    skew[1, 8:24, :] = by_time(z_lab - lse)
    offsets = [8 - u for u in range(8)]
    group24 = jnp.broadcast_to(group, (24, 128))
    blank = pick_rows(skew.at[0], offsets, group24)
    lab = pick_rows(skew.at[1], offsets, group24)

    first_u = group == 0
    last_u = group == 7
    alpha = jnp.where(first_u, 0.0, NEG).astype(F32)
    alphas = [alpha]
    for d in range(1, 23):
        stay = alpha + blank[d - 1:d]
        step = jnp.where(first_u, NEG, pltpu.roll(alpha + lab[d - 1:d], 8, 1))
        alpha = logaddexp(stay, step)
        alphas.append(alpha)
    alphas.append(jnp.full((1, 128), NEG, F32))
    bound = jnp.where(group == n_labels, 0.0, NEG).astype(F32)
    beta = bound
    nexts, ups = [None] * 24, [None] * 24
    nexts[23] = ups[23] = jnp.full((1, 128), NEG, F32)
    for d in range(22, -1, -1):
        up = jnp.where(last_u, NEG, pltpu.roll(beta, 120, 1))
        nexts[d], ups[d] = beta, up
        new = logaddexp(beta + blank[d:d + 1], up + lab[d:d + 1])
        beta = jnp.where(d - group >= n_frames, bound, new)
    log_p = jnp.where(lane < 8, beta, 0.0)
    for shift in (8, 16, 32, 64):
        log_p = log_p + pltpu.roll(log_p, shift, 1)

    alphas = jnp.concatenate(alphas, axis=0)
    nexts = jnp.concatenate(nexts, axis=0)
    ups = jnp.concatenate(ups, axis=0)
    frame = iota((24, 128), 0) - group24
    ok = (frame >= 0) & (frame < n_frames)
    occ_b = jnp.where(ok, jnp.exp(jnp.minimum(alphas + blank + nexts - log_p, 0.0)), 0.0)
    occ_l = jnp.where(ok & (group24 < 7), jnp.exp(jnp.minimum(alphas + lab + ups - log_p, 0.0)), 0.0)
    skew[0, 0:24, :] = occ_b
    skew[1, 0:24, :] = occ_l
    offsets = list(range(8))
    low = jnp.broadcast_to(lane < 64, (8, 128))

    def by_tile(x):
        return jnp.where(low, x[0:8], pltpu.roll(x[8:16], 64, 1))

    stats[me, 0:8, :] = lse
    stats[me, 8:16, :] = by_tile(pick_rows(skew.at[0], offsets, group24))
    stats[me, 16:24, :] = by_tile(pick_rows(skew.at[1], offsets, group24))
    stats[me, 24:32, :] = jnp.broadcast_to(log_p, (8, 128))


def grad_logits(z, stats, block, lab, first_id, col0=0, has_blank=None):
    rows, cols = z.shape
    ids = iota((rows, 128), 0) + first_id
    tiles = []
    for k in range(cols // 128):
        kk = k + col0
        lse = stats[block, kk:kk + 1, :]
        occ_b = stats[block, 8 + kk:9 + kk, :]
        occ_l = stats[block, 16 + kk:17 + kk, :]
        tile = jnp.exp(z[:, k * 128:(k + 1) * 128] - lse) * (occ_b + occ_l)
        tile = tile - jnp.where(ids == lab, occ_l, 0.0)
        head = tile[0:16] - jnp.where(ids[0:16] == 0, occ_b, 0.0)
        tiles.append(jnp.concatenate([head, tile[16:]], axis=0).astype(BF16))
    return jnp.concatenate(tiles, axis=1)


def own_lengths(ref, scratch, me):
    scratch[...] = jnp.zeros_like(scratch)
    scratch[:, 0:64] = ref[...]
    x = pltpu.roll(scratch[...], lax.rem(128 - 8 * me, 128), 1)
    x = jnp.where(iota((1, 128), 1) < 8, x, 0)
    for shift in (8, 16, 32, 64):
        x = x + pltpu.roll(x, shift, 1)
    return x


def spread_labels(labels, scratch, lab):
    scratch[...] = jnp.full_like(scratch, -1)
    scratch[0:7, 0:64] = labels[...]
    scratch[0:7, 64:128] = labels[...]
    x = pltpu.roll(scratch[...], 0, 1, stride=8, stride_axis=0)
    keep = lax.rem(iota((8, 128), 1) // 8, 8) == iota((8, 128), 0)
    for d in range(N_DEV):
        turned = pltpu.roll(x, 128 - 8 * d, 1) if d else x
        lab[d:d + 1, :] = jnp.sum(jnp.where(keep, turned, 0), axis=0, keepdims=True)


def main_kernel(enc3, g, w_enc, w_pred, w_hbm, labels, frame_len, label_len,
                gw_buf, da_all, dc_all, f_all, stats,
                enc, w_out, wt, ht, sel, act, wet, wpt, dh, dzs, skew, lab, lab_x, len_x, load_sem,
                a2a_s, a2a_r, f_s, f_r, st_s, st_r, gw_s, gw_r, da_s, da_r, dc_s, dc_r):
    p = Peers()
    me = p.me
    barrier = pltpu.get_barrier_semaphore()
    for k in range(1, N_DEV):
        pl.semaphore_signal(barrier, inc=1, device_id=p.target(lax.rem(me + k, N_DEV)),
                            device_id_type=pl.DeviceIdType.MESH)
    loads = []
    for k in range(4):
        cols = slice(k * 1024, (k + 1) * 1024)
        loads.append(pltpu.make_async_copy(w_hbm.at[:, cols], w_out.at[:, cols], load_sem.at[k]))
        loads[-1].start()
    enc[...] = enc3[...].reshape(128, DIM)
    pl.semaphore_wait(barrier, N_DEV - 1)

    def rows16(i):
        return pl.ds(pl.multiple_of(i * 16, 16), 16)

    copies = []
    for k in range(1, N_DEV):
        to = lax.rem(me + k, N_DEV)
        copies.append(remote(enc.at[rows16(to), :], f_all.at[to, rows16(me), :], a2a_s.at[k], a2a_r.at[k], p.target(to)))
    for c in copies:
        c.start()
    f_all[me, rows16(me), :] = enc[rows16(me), :]

    ident = eye(256)
    transpose_into(wet, w_enc, ident)
    transpose_into(wpt, w_pred, ident)
    row = iota((192, LANES), 0)
    col = iota((192, LANES), 1)
    t_id = col // 128 + 8 * (lax.rem(col, 128) // 64)
    u_id = lax.rem(col // 8, 8)
    b_id = lax.rem(col, 8)
    a_row = 2 * (row // 16) + lax.rem(row, 2)
    a_b = lax.rem(row // 2, 8)
    c_row = row - 128
    hit = jnp.where(row < 128, jnp.where((a_row == t_id) & (a_b == b_id), 1.0, 0.0),
                    jnp.where((c_row // 8 == b_id) & (lax.rem(c_row, 8) == u_id), 1.0, 0.0))
    sel[...] = hit.astype(BF16)
    spread_labels(labels, lab_x, lab)
    n_frames = own_lengths(frame_len, len_x, me)
    n_labels = own_lengths(label_len, len_x, me)
    for d in range(N_DEV):
        act[d, :, 128:192] = dot_nt(wpt[...], g[d * 64:(d + 1) * 64, :]).astype(BF16)

    def transpose_out(c, _):
        lo = pl.multiple_of(c * CHUNK, CHUNK)
        wt[pl.ds(lo, CHUNK), :] = dot_nt(ident, w_out[:, pl.ds(lo, CHUNK)]).astype(BF16)
        return 0

    for k in range(4):
        loads[k].wait()
        lax.fori_loop(4 * k, 4 * k + 4, transpose_out, 0, unroll=4)

    for k in range(1, N_DEV):
        src = lax.rem(me + N_DEV - k, N_DEV)
        remote(enc.at[rows16(me), :], f_all.at[me, rows16(src), :], a2a_s.at[k], a2a_r.at[k], p.target(src)).wait_recv()

    f_gather = Direct(p, lambda d: f_all.at[me], lambda i: f_all.at[i], f_s, f_r)
    f_gather.start()

    def hidden(d):
        act[d, :, 0:128] = dot_nt(wet[...], f_all[d]).astype(BF16)
        ht[d] = jnp.tanh(dot_nn(act[d], sel[...])).astype(BF16)

    hidden(me)
    lab_own = lab[pl.ds(me, 1), :]
    lab_row = jnp.concatenate([lab_own] * 8, axis=1)

    def forward(c, carry):
        top, total, z_lab = carry
        lo = pl.multiple_of(c * CHUNK, CHUNK)
        z = dot_nn(wt[pl.ds(lo, CHUNK), :], ht[me]).reshape(CHUNK // 8, 8, LANES)
        new = jnp.maximum(top, jnp.max(z, axis=0))
        total = total * jnp.exp(top - new) + jnp.sum(jnp.exp(z - new[None]), axis=0)
        ids = iota((CHUNK // 8, 8, LANES), 0) * 8 + iota((CHUNK // 8, 8, LANES), 1) + lo
        z_lab = z_lab + jnp.sum(jnp.where(ids == lab_row[None], z, 0.0), axis=0)
        return new, total, z_lab

    start = (jnp.full((8, LANES), NEG, F32), jnp.zeros((8, LANES), F32), jnp.zeros((8, LANES), F32))
    top, total, z_lab = lax.fori_loop(0, VOCAB // CHUNK, forward, start, unroll=4)
    peak = jnp.max(top, axis=0, keepdims=True)
    lse = peak + jnp.log(jnp.sum(total * jnp.exp(top - peak), axis=0, keepdims=True))
    z_lab = jnp.sum(z_lab, axis=0, keepdims=True)
    z_blank = dot_nn(wt[0:16, :], ht[me])[0:1]

    def tiles(x):
        return jnp.concatenate([x[:, k * 128:(k + 1) * 128] for k in range(8)], axis=0)

    lattice(tiles(lse), tiles(z_blank), tiles(z_lab), n_frames, n_labels, me, skew, stats)
    st_gather = Direct(p, lambda d: stats.at[me], lambda i: stats.at[i], st_s, st_r)
    st_gather.start()

    f_gather.wait_recv()

    def hidden_other(k, _):
        hidden(lax.rem(me + k, N_DEV))
        return 0

    lax.fori_loop(1, N_DEV, hidden_other, 0, unroll=7)
    st_gather.wait_recv()

    mine = 2 * p.diag
    pair = Pair(p, gw_buf, mine, 2 - mine, gw_s, gw_r)
    own_set = mine + p.core
    dh[...] = jnp.zeros_like(dh)

    def chunk(c, _):
        n = own_set * 4 + c
        first = pl.multiple_of(n * CHUNK, CHUNK)
        rows = wt[pl.ds(first, CHUNK), :]
        z = dot_nn(rows, ht[0])
        for d in range(N_DEV):
            z_next = dot_nn(rows, ht[d + 1]) if d + 1 < N_DEV else None
            dz = grad_logits(z, stats, d, lab[d:d + 1, :], first)
            dzs[d] = dz
            part = dot_nt(ht[d], dz)
            gw_buf[n] = part if d == 0 else gw_buf[n] + part
            z = z_next
        pair.start(c)
        dh[...] += dot_nn(w_out[:, pl.ds(first, CHUNK)], dzs[me])
        return 0

    lax.fori_loop(0, 4, chunk, 0)

    def backward(i, _):
        lo = pl.multiple_of(lax.rem(2 * own_set + 2 + i, 8) * 512, 512)
        z = dot_nn(wt[pl.ds(lo, 512), :], ht[me])
        dz = grad_logits(z, stats, me, lab_own, lo)
        dh[...] += dot_nn(w_out[:, pl.ds(lo, 512)], dz)
        return 0

    lax.fori_loop(0, 6, backward, 0, unroll=2)
    h32 = ht[me].astype(F32)
    dp = (dh[...] * (1.0 - h32 * h32)).astype(BF16)
    sums = dot_nt(dp, sel[...])
    da_all[me] = sums[:, 0:128].astype(BF16)
    dc_all[me] = jnp.concatenate([sums[0:320, 128:192], sums[320:640, 128:192]], axis=1)
    da_relay = Relay(p, lambda e: da_all.at[e], lambda e, h: da_all.at[e, pl.ds(h * 320, 320), :], da_s, da_r)
    dc_relay = Relay(p, lambda e: dc_all.at[e], lambda e, h: dc_all.at[e, pl.ds(h * 160, 160), :], dc_s, dc_r)
    da_relay.start()
    dc_relay.start()
    for c in range(4):
        pair.pass_on(c)
    da_relay.pass_on()
    dc_relay.pass_on()
    da_relay.pass_diagonal()
    dc_relay.pass_diagonal()
    for c in range(4):
        pair.finish(c)
    da_relay.finish()
    dc_relay.finish()
    for c in copies:
        c.wait_send()
    f_gather.wait_send()
    st_gather.wait_send()


def final_kernel(gw_buf, da_all, dc_all, f_all, stats, g, w_enc, loss, grad_enc, gw_enc, gw_pred, gw_out, ft, gt, out_sem):
    me = lax.axis_index('seq')
    flush = []
    for n in range(VOCAB // CHUNK):
        flush.append(pltpu.make_async_copy(gw_buf.at[n], gw_out.at[:, n * CHUNK:(n + 1) * CHUNK], out_sem.at[n]))
        flush[-1].start()
    ident = eye(256)
    for d in range(N_DEV):
        for lo in range(0, DIM, 256):
            width = min(256, DIM - lo)
            ft[lo:lo + width, d * 128:(d + 1) * 128] = dot_nt(ident[:width, :width], f_all[d, :, lo:lo + width]).astype(BF16)
    transpose_into(gt, g, ident)
    da = jnp.concatenate([da_all[d] for d in range(N_DEV)], axis=1)
    gw_enc[...] = dot_nt(ft[...], da)
    pick = jnp.where(iota((16, 128), 1) == iota((16, 128), 0) + me * 16, 1.0, 0.0).astype(BF16)
    mine = jnp.concatenate([dot_nt(pick, da_all[d]).astype(BF16) for d in range(N_DEV)], axis=0)
    grad_enc[...] = dot_nt(mine, w_enc[...]).reshape(64, 2, DIM).astype(BF16)
    total = jnp.zeros((1, 128), F32)
    for d in range(N_DEV):
        own = jnp.where(iota((1, 128), 1) < 8, stats[d, 24:25, :], 0.0)
        total = total - (pltpu.roll(own, 8 * d, 1) if d else own)
    loss[...] = total[:, 0:64]
    dc = jnp.concatenate([jnp.concatenate([dc_all[d, :, 0:64], dc_all[d, :, 64:128]], axis=0) for d in range(N_DEV)], axis=1)
    gw_pred[...] = dot_nt(gt[...], dc.astype(BF16))
    for copy in flush:
        copy.wait()


def vmem():
    return pl.BlockSpec(memory_space=pltpu.VMEM)


def solution(mesh):
    dma = pltpu.SemaphoreType.DMA

    def local_fn(enc_out, pred_out, w_enc, w_pred, w_out, labels, frame_len, label_len):
        n_utt = pred_out.shape[0]
        g = pred_out.reshape(8 * n_utt, DIM)
        hbm = pl.BlockSpec(memory_space=pl.ANY)
        handed = pl.pallas_call(
            main_kernel,
            out_shape=(pltpu.VMEM((16, DIM, CHUNK), F32), pltpu.VMEM((8, DIM, 128), BF16),
                       pltpu.VMEM((8, DIM // 2, 128), F32), pltpu.VMEM((8, 128, DIM), BF16),
                       pltpu.VMEM((8, 32, 128), F32)),
            in_specs=[vmem()] * 4 + [hbm] + [vmem()] * 3,
            out_specs=(vmem(),) * 5,
            scratch_shapes=[pltpu.VMEM((128, DIM), BF16), pltpu.VMEM((DIM, VOCAB), BF16),
                            pltpu.VMEM((VOCAB, DIM), BF16), pltpu.VMEM((8, DIM, LANES), BF16),
                            pltpu.VMEM((192, LANES), BF16), pltpu.VMEM((8, DIM, 192), BF16),
                            pltpu.VMEM((DIM, DIM), BF16), pltpu.VMEM((DIM, DIM), BF16),
                            pltpu.VMEM((DIM, LANES), F32), pltpu.VMEM((8, CHUNK, LANES), BF16),
                            pltpu.VMEM((2, 40, 128), F32), pltpu.VMEM((8, 128), jnp.int32),
                            pltpu.VMEM((8, 128), jnp.int32), pltpu.VMEM((1, 128), jnp.int32), dma((4,)),
                            dma((8,)), dma((8,)), dma((8,)), dma((8,)), dma((8,)), dma((8,)),
                            dma((4, 5)), dma((4, 5)), dma((9,)), dma((9,)), dma((9,)), dma((9,))],
            compiler_params=pltpu.CompilerParams(collective_id=0, has_side_effects=True, vmem_limit_bytes=MAIN_VMEM),
        )(enc_out, g, w_enc, w_pred, w_out, labels.T, frame_len.reshape(1, n_utt), label_len.reshape(1, n_utt))
        loss, grad_enc, gw_enc, gw_pred, gw_out = pl.pallas_call(
            final_kernel,
            out_shape=(jax.ShapeDtypeStruct((1, n_utt), F32),
                       jax.ShapeDtypeStruct(enc_out.shape, BF16),
                       jax.ShapeDtypeStruct((DIM, DIM), F32),
                       jax.ShapeDtypeStruct((DIM, DIM), F32),
                       jax.ShapeDtypeStruct((DIM, VOCAB), F32)),
            in_specs=[vmem()] * 7,
            out_specs=(vmem(), vmem(), vmem(), vmem(), hbm),
            scratch_shapes=[pltpu.VMEM((DIM, LANES), BF16), pltpu.VMEM((DIM, 512), BF16), dma((16,))],
            compiler_params=pltpu.CompilerParams(vmem_limit_bytes=LAST_VMEM),
        )(*handed, g, w_enc)
        return loss.reshape(n_utt), grad_enc, gw_enc, gw_pred, gw_out

    in_specs = (P('dp', 'seq', None), P('dp', None, None), P(None, None), P(None, None), P(None, None), P('dp', None), P('dp'), P('dp'))
    out_specs = (P('dp'), P('dp', 'seq', None), P('dp', None), P('dp', None), P('dp', None))
    return jax.shard_map(local_fn, mesh=mesh, in_specs=in_specs, out_specs=out_specs, check_vma=False)
```

```python
import jax
import jax.numpy as jnp
from jax import lax
from jax.experimental import pallas as pl
from jax.experimental.pallas import tpu as pltpu
from jax.sharding import PartitionSpec as P

NEG = -1.0e30
F32 = jnp.float32
BF16 = jnp.bfloat16
N_DEV = 8
DIM = 640
VOCAB = 4096
LANES = 1024
CHUNK = 256
MAIN_VMEM = 52_600_000
LAST_VMEM = 1_000_000
OCT, DIAGS, HALF, TILE, WIDE, MID = 8, 24, 64, 128, 192, 320


def dot_nn(lhs, rhs):
    return lax.dot_general(lhs, rhs, (((1,), (0,)), ((), ())), preferred_element_type=F32)


def dot_nt(lhs, rhs):
    return lax.dot_general(lhs, rhs, (((1,), (1,)), ((), ())), preferred_element_type=F32)


def iota(shape, axis):
    return lax.broadcasted_iota(jnp.int32, shape, axis)


def eye(size):
    return jnp.where(iota((size, size), 0) == iota((size, size), 1), 1.0, 0.0).astype(BF16)


def transpose_into(dst, src, ident):
    cols = src.shape[1]
    for lo in range(0, cols, CHUNK):
        width = min(CHUNK, cols - lo)
        dst[lo:lo + width, :] = dot_nt(ident[:width, :width], src[:, lo:lo + width]).astype(BF16)


def logaddexp(a, b):
    top = jnp.maximum(a, b)
    return top + jnp.log(1.0 + jnp.exp(-jnp.abs(a - b)))


class Peers:
    def __init__(self):
        self.dp = lax.axis_index('dp')
        self.me = lax.axis_index('seq')
        core = lax.rem(self.me, 2)
        col = lax.rem(self.me // 2, 2)
        row = self.me // 4
        self.core = core
        self.diag = lax.rem(row + col, 2)
        self.pp = row * 4 + col * 2 + (1 - core)
        self.px = row * 4 + (1 - col) * 2 + core
        self.py = (1 - row) * 4 + col * 2 + core
        self.pd = (1 - row) * 4 + (1 - col) * 2 + core
        self.px_p = row * 4 + (1 - col) * 2 + (1 - core)
        self.py_p = (1 - row) * 4 + col * 2 + (1 - core)
        self.pd_p = (1 - row) * 4 + (1 - col) * 2 + (1 - core)

    def target(self, seq):
        return (self.dp, seq)


def remote(src, dst, send_sem, recv_sem, device):
    return pltpu.make_async_remote_copy(src_ref=src, dst_ref=dst, send_sem=send_sem, recv_sem=recv_sem,
                                        device_id=device, device_id_type=pl.DeviceIdType.MESH)


class Relay:
    def __init__(self, peers, view, half, send_sem, recv_sem):
        self.p = peers
        self.view = view
        self.half = half
        self.ssem = send_sem
        self.rsem = recv_sem

    def copy(self, kind, block, device):
        return remote(block, block, self.ssem.at[kind], self.rsem.at[kind], self.p.target(device))

    def stage(self, number, x, y, d):
        p = self.p
        if number == 0:
            base, pairs = 0, ((p.px, self.view(p.me)), (p.py, self.view(p.me)), (p.pp, self.view(x)))
        elif number == 1:
            base, pairs = 3, ((p.py, self.half(x, 0)), (p.px, self.half(y, 1)), (p.pp, self.view(x)), (p.pp, self.view(y)))
        else:
            base, pairs = 7, ((p.pp, self.half(d, 0)), (p.pp, self.half(d, 1)))
        return [self.copy(base + i, block, device) for i, (device, block) in enumerate(pairs)]

    def start(self):
        for copy in self.stage(0, self.p.me, None, None):
            copy.start()

    def pass_on(self):
        p = self.p
        from_x = self.copy(0, self.view(p.px), p.px)
        from_y = self.copy(1, self.view(p.py), p.py)
        to_y, to_x, x_over, y_over = self.stage(1, p.px, p.py, None)
        from_x.wait_recv()
        to_y.start()
        x_over.start()
        from_y.wait_recv()
        to_x.start()
        y_over.start()

    def pass_diagonal(self):
        p = self.p
        self.copy(3, self.half(p.pd, 0), p.py).wait_recv()
        self.copy(4, self.half(p.pd, 1), p.px).wait_recv()
        for copy in self.stage(2, None, None, p.pd):
            copy.start()

    def finish(self):
        p = self.p
        self.stage(0, p.pp, None, None)[2].wait_recv()
        for copy in self.stage(1, p.px_p, p.py_p, None)[2:] + self.stage(2, None, None, p.pd_p):
            copy.wait_recv()
        for copy in self.stage(0, p.me, None, None) + self.stage(1, p.px, p.py, None) + self.stage(2, None, None, p.pd):
            copy.wait_send()


class Pair:
    def __init__(self, peers, buf, mine, other, send_sem, recv_sem):
        self.p = peers
        self.buf = buf
        self.mine = mine
        self.other = other
        self.ssem = send_sem
        self.rsem = recv_sem

    def copy(self, c, kind, block, device):
        return remote(block, block, self.ssem.at[c, kind], self.rsem.at[c, kind], self.p.target(device))

    def half(self, base, core, c, h):
        return self.buf.at[(base + core) * 4 + c, h * MID:(h + 1) * MID, :]

    def start(self, c):
        p = self.p
        self.copy(c, 1, self.half(self.mine, p.core, c, 0), p.px).start()
        self.copy(c, 2, self.half(self.mine, p.core, c, 1), p.py).start()
        self.copy(c, 0, self.buf.at[(self.mine + p.core) * 4 + c], p.pp).start()

    def pass_on(self, c):
        p = self.p
        low = self.half(self.other, p.core, c, 0)
        high = self.half(self.other, p.core, c, 1)
        self.copy(c, 1, low, p.px).wait_recv()
        self.copy(c, 3, low, p.pp).start()
        self.copy(c, 2, high, p.py).wait_recv()
        self.copy(c, 4, high, p.pp).start()

    def finish(self, c):
        p = self.p
        twin = 1 - p.core
        self.copy(c, 0, self.buf.at[(self.mine + twin) * 4 + c], p.pp).wait_recv()
        self.copy(c, 3, self.half(self.other, twin, c, 0), p.pp).wait_recv()
        self.copy(c, 4, self.half(self.other, twin, c, 1), p.pp).wait_recv()
        self.copy(c, 0, self.buf.at[(self.mine + p.core) * 4 + c], p.pp).wait_send()
        self.copy(c, 1, self.half(self.mine, p.core, c, 0), p.px).wait_send()
        self.copy(c, 2, self.half(self.mine, p.core, c, 1), p.py).wait_send()
        self.copy(c, 3, self.half(self.other, p.core, c, 0), p.pp).wait_send()
        self.copy(c, 4, self.half(self.other, p.core, c, 1), p.pp).wait_send()


class Direct:
    def __init__(self, peers, src, dst, send_sem, recv_sem):
        self.p = peers
        self.src = src
        self.dst = dst
        self.ssem = send_sem
        self.rsem = recv_sem

    def copy(self, k, to, source):
        return remote(self.src(to), self.dst(source), self.ssem.at[k], self.rsem.at[k], self.p.target(to))

    def start(self):
        for k in range(1, N_DEV):
            self.copy(k, lax.rem(self.p.me + k, N_DEV), self.p.me).start()

    def wait_recv(self):
        for k in range(1, N_DEV):
            self.copy(k, lax.rem(self.p.me + k, N_DEV), lax.rem(self.p.me + N_DEV - k, N_DEV)).wait_recv()

    def wait_send(self):
        for k in range(1, N_DEV):
            self.copy(k, lax.rem(self.p.me + k, N_DEV), self.p.me).wait_send()


def pick_rows(ref, offsets, group):
    out = None
    for u, off in enumerate(offsets):
        part = ref[off:off + DIAGS, :]
        out = part if out is None else jnp.where(group == u, part, out)
    return out


def lattice(lse, z_blank, z_lab, n_frames, n_labels, me, skew, stats):
    lane = iota((1, TILE), 1)
    group = lax.rem(lane // OCT, OCT)

    def by_time(x):
        return jnp.concatenate([x, pltpu.roll(x, HALF, 1)], axis=0)

    skew[...] = jnp.zeros_like(skew)
    skew[0, OCT:DIAGS, :] = by_time(z_blank - lse)
    skew[1, OCT:DIAGS, :] = by_time(z_lab - lse)
    offsets = [OCT - u for u in range(OCT)]
    group24 = jnp.broadcast_to(group, (DIAGS, TILE))
    blank = pick_rows(skew.at[0], offsets, group24)
    lab = pick_rows(skew.at[1], offsets, group24)

    first_u = group == 0
    last_u = group == 7
    alpha = jnp.where(first_u, 0.0, NEG).astype(F32)
    alphas = [alpha]
    for d in range(1, 23):
        stay = alpha + blank[d - 1:d]
        step = jnp.where(first_u, NEG, pltpu.roll(alpha + lab[d - 1:d], OCT, 1))
        alpha = logaddexp(stay, step)
        alphas.append(alpha)
    alphas.append(jnp.full((1, TILE), NEG, F32))
    bound = jnp.where(group == n_labels, 0.0, NEG).astype(F32)
    beta = bound
    nexts, ups = [None] * DIAGS, [None] * DIAGS
    nexts[23] = ups[23] = jnp.full((1, TILE), NEG, F32)
    for d in range(22, -1, -1):
        up = jnp.where(last_u, NEG, pltpu.roll(beta, 120, 1))
        nexts[d], ups[d] = beta, up
        new = logaddexp(beta + blank[d:d + 1], up + lab[d:d + 1])
        beta = jnp.where(d - group >= n_frames, bound, new)
    log_p = jnp.where(lane < OCT, beta, 0.0)
    for shift in (OCT, 16, 32, HALF):
        log_p = log_p + pltpu.roll(log_p, shift, 1)

    alphas = jnp.concatenate(alphas, axis=0)
    nexts = jnp.concatenate(nexts, axis=0)
    ups = jnp.concatenate(ups, axis=0)
    frame = iota((DIAGS, TILE), 0) - group24
    ok = (frame >= 0) & (frame < n_frames)
    occ_b = jnp.where(ok, jnp.exp(jnp.minimum(alphas + blank + nexts - log_p, 0.0)), 0.0)
    occ_l = jnp.where(ok & (group24 < 7), jnp.exp(jnp.minimum(alphas + lab + ups - log_p, 0.0)), 0.0)
    skew[0, 0:DIAGS, :] = occ_b
    skew[1, 0:DIAGS, :] = occ_l
    offsets = list(range(OCT))
    low = jnp.broadcast_to(lane < HALF, (OCT, TILE))

    def by_tile(x):
        return jnp.where(low, x[0:OCT], pltpu.roll(x[OCT:16], HALF, 1))

    stats[me, 0:OCT, :] = lse
    stats[me, OCT:16, :] = by_tile(pick_rows(skew.at[0], offsets, group24))
    stats[me, 16:DIAGS, :] = by_tile(pick_rows(skew.at[1], offsets, group24))
    stats[me, DIAGS:32, :] = jnp.broadcast_to(log_p, (OCT, TILE))


def grad_logits(z, stats, block, lab, first_id, col0=0, has_blank=None):
    rows, cols = z.shape
    ids = iota((rows, TILE), 0) + first_id
    tiles = []
    for k in range(cols // TILE):
        kk = k + col0
        lse = stats[block, kk:kk + 1, :]
        occ_b = stats[block, OCT + kk:9 + kk, :]
        occ_l = stats[block, 16 + kk:17 + kk, :]
        tile = jnp.exp(z[:, k * TILE:(k + 1) * TILE] - lse) * (occ_b + occ_l)
        tile = tile - jnp.where(ids == lab, occ_l, 0.0)
        head = tile[0:16] - jnp.where(ids[0:16] == 0, occ_b, 0.0)
        tiles.append(jnp.concatenate([head, tile[16:]], axis=0).astype(BF16))
    return jnp.concatenate(tiles, axis=1)


def own_lengths(ref, scratch, me):
    scratch[...] = jnp.zeros_like(scratch)
    scratch[:, 0:HALF] = ref[...]
    x = pltpu.roll(scratch[...], lax.rem(TILE - OCT * me, TILE), 1)
    x = jnp.where(iota((1, TILE), 1) < OCT, x, 0)
    for shift in (OCT, 16, 32, HALF):
        x = x + pltpu.roll(x, shift, 1)
    return x


def spread_labels(labels, scratch, lab):
    scratch[...] = jnp.full_like(scratch, -1)
    scratch[0:7, 0:HALF] = labels[...]
    scratch[0:7, HALF:TILE] = labels[...]
    x = pltpu.roll(scratch[...], 0, 1, stride=OCT, stride_axis=0)
    keep = lax.rem(iota((OCT, TILE), 1) // OCT, OCT) == iota((OCT, TILE), 0)
    for d in range(N_DEV):
        turned = pltpu.roll(x, TILE - OCT * d, 1) if d else x
        lab[d:d + 1, :] = jnp.sum(jnp.where(keep, turned, 0), axis=0, keepdims=True)


def main_kernel(enc3, g_hbm, we_hbm, wp_hbm, w_hbm, labels, frame_len, label_len,
                loss, grad_enc, gw_enc, gw_pred, gw_buf,
                enc, g, w_enc, w_out, wt, ht, zs, sel, act, c_all, wet, da_all, dc_all, f_all, stats, skew, lab, lab_x, len_x,
                load_sem, a2a_s, a2a_r, st_s, st_r, gw_s, gw_r, f_s, f_r, da_s, da_r, dc_s, dc_r):
    p = Peers()
    me = p.me
    barrier = pltpu.get_barrier_semaphore()
    for k in range(1, N_DEV):
        pl.semaphore_signal(barrier, inc=1, device_id=p.target(lax.rem(me + k, N_DEV)),
                            device_id_type=pl.DeviceIdType.MESH)
    w_pred, wpt = ht.at[0, :, 0:DIM], ht.at[1, :, 0:DIM]
    loads = [(wp_hbm, w_pred), (g_hbm, g), (we_hbm, w_enc)]
    for lo in range(0, VOCAB, LANES):
        loads.append((w_hbm.at[:, lo:lo + LANES], w_out.at[:, lo:lo + LANES]))
    loads = [pltpu.make_async_copy(src, dst, load_sem.at[k]) for k, (src, dst) in enumerate(loads)]
    for copy in loads:
        copy.start()
    enc[...] = enc3[...].reshape(TILE, DIM)
    pl.semaphore_wait(barrier, N_DEV - 1)

    def rows16(i):
        return pl.ds(pl.multiple_of(i * 16, 16), 16)

    copies = []
    for k in range(1, N_DEV):
        to = lax.rem(me + k, N_DEV)
        copies.append(remote(enc.at[rows16(to), :], f_all.at[to, rows16(me), :], a2a_s.at[k], a2a_r.at[k], p.target(to)))
    for copy in copies:
        copy.start()
    f_all[me, rows16(me), :] = enc[rows16(me), :]

    ident = eye(CHUNK)
    row = iota((WIDE, LANES), 0)
    col = iota((WIDE, LANES), 1)
    t_id = col // TILE + OCT * (lax.rem(col, TILE) // HALF)
    u_id = lax.rem(col // OCT, OCT)
    b_id = lax.rem(col, OCT)
    a_row = 2 * (row // 16) + lax.rem(row, 2)
    a_b = lax.rem(row // 2, OCT)
    c_row = row - TILE
    hit = jnp.where(row < TILE, jnp.where((a_row == t_id) & (a_b == b_id), 1.0, 0.0),
                    jnp.where((c_row // OCT == b_id) & (lax.rem(c_row, OCT) == u_id), 1.0, 0.0))
    sel[...] = hit.astype(BF16)
    spread_labels(labels, lab_x, lab)
    n_frames = own_lengths(frame_len, len_x, me)
    n_labels = own_lengths(label_len, len_x, me)
    first_loads, last_loads = loads[:3], loads[3:]
    for copy in first_loads:
        copy.wait()
    transpose_into(wpt, w_pred, ident)
    transpose_into(wet, w_enc, ident)
    c_cols = dot_nt(wpt[...], g[...]).astype(BF16)
    for d in range(N_DEV):
        c_all[d] = c_cols[:, d * HALF:(d + 1) * HALF]

    def transpose_out(c, _):
        lo = pl.multiple_of(c * CHUNK, CHUNK)
        wt[pl.ds(lo, CHUNK), :] = dot_nt(ident, w_out[:, pl.ds(lo, CHUNK)]).astype(BF16)
        return 0

    for k, copy in enumerate(last_loads):
        copy.wait()
        lax.fori_loop(4 * k, 4 * k + 4, transpose_out, 0, unroll=4)

    for k in range(1, N_DEV):
        src = lax.rem(me + N_DEV - k, N_DEV)
        remote(enc.at[rows16(me), :], f_all.at[me, rows16(src), :], a2a_s.at[k], a2a_r.at[k], p.target(src)).wait_recv()

    f_relay = Relay(p, lambda e: f_all.at[e], lambda e, h: f_all.at[e, h * HALF:(h + 1) * HALF, :], f_s, f_r)
    f_relay.start()

    def hidden(d, slot):
        act[slot, :, 0:TILE] = dot_nt(wet[...], f_all[d]).astype(BF16)
        act[slot, :, TILE:WIDE] = c_all[d]
        ht[d] = jnp.tanh(dot_nn(act[slot], sel[...])).astype(BF16)

    hidden(me, 0)
    lab_own = lab[pl.ds(me, 1), :]
    lab_row = jnp.concatenate([lab_own] * OCT, axis=1)

    def forward(c, carry):
        top, total, z_lab = carry
        lo = pl.multiple_of(c * CHUNK, CHUNK)
        z = dot_nn(wt[pl.ds(lo, CHUNK), :], ht[me])
        zs[pl.ds(lo, CHUNK), :] = z
        z = z.reshape(CHUNK // OCT, OCT, LANES)
        new = jnp.maximum(top, jnp.max(z, axis=0))
        total = total * jnp.exp(top - new) + jnp.sum(jnp.exp(z - new[None]), axis=0)
        ids = iota(z.shape, 0) * OCT + iota(z.shape, 1) + lo
        z_lab = z_lab + jnp.sum(jnp.where(ids == lab_row[None], z, 0.0), axis=0)
        return new, total, z_lab

    carry = (jnp.full((OCT, LANES), NEG, F32), jnp.zeros((OCT, LANES), F32), jnp.zeros((OCT, LANES), F32))
    carry = lax.fori_loop(0, OCT, forward, carry, unroll=4)
    f_relay.pass_on()
    top, total, z_lab = lax.fori_loop(OCT, 16, forward, carry, unroll=4)
    f_relay.pass_diagonal()
    peak = jnp.max(top, axis=0, keepdims=True)
    lse = peak + jnp.log(jnp.sum(total * jnp.exp(top - peak), axis=0, keepdims=True))
    z_lab = jnp.sum(z_lab, axis=0, keepdims=True)
    z_blank = zs[0:1, :]

    def tiles(x):
        return jnp.concatenate([x[:, k * TILE:(k + 1) * TILE] for k in range(OCT)], axis=0)

    lattice(tiles(lse), tiles(z_blank), tiles(z_lab), n_frames, n_labels, me, skew, stats)
    st_gather = Direct(p, lambda d: stats.at[me], lambda i: stats.at[i], st_s, st_r)
    st_gather.start()

    mine = 2 * p.diag
    own_set = mine + p.core
    slots = [own_set * 4 + j for j in range(4)]
    for slot in slots:
        gw_buf[slot] = jnp.zeros((DIM, CHUNK), F32)

    def backward(i, _):
        lo = pl.multiple_of(i * 512, 512)
        dz = grad_logits(zs[pl.ds(lo, 512), :], stats, me, lab_own, lo)
        part = dot_nn(w_out[:, pl.ds(lo, 512)], dz)
        for j, slot in enumerate(slots):
            gw_buf[slot] += part[:, j * CHUNK:(j + 1) * CHUNK]
        return 0

    lax.fori_loop(0, OCT, backward, 0, unroll=2)
    sums = None
    for j, slot in enumerate(slots):
        cols = slice(j * CHUNK, (j + 1) * CHUNK)
        h32 = ht[me, :, cols].astype(F32)
        dp = (gw_buf[slot] * (1.0 - h32 * h32)).astype(BF16)
        part = dot_nt(dp, sel[:, cols])
        sums = part if sums is None else sums + part
    da_all[me] = sums[:, 0:TILE].astype(BF16)
    dc_all[me] = jnp.concatenate([sums[0:MID, TILE:WIDE], sums[MID:DIM, TILE:WIDE]], axis=1)
    da_relay = Relay(p, lambda e: da_all.at[e], lambda e, h: da_all.at[e, h * MID:(h + 1) * MID, :], da_s, da_r)
    dc_relay = Relay(p, lambda e: dc_all.at[e], lambda e, h: dc_all.at[e, h * 160:(h + 1) * 160, :], dc_s, dc_r)
    da_relay.start()
    dc_relay.start()

    f_relay.finish()
    for k in range(1, N_DEV):
        hidden(lax.rem(me + k, N_DEV), k % 2)
    st_gather.wait_recv()
    pair = Pair(p, gw_buf, mine, 2 - mine, gw_s, gw_r)

    def chunk(c, _):
        n = own_set * 4 + c
        first = pl.multiple_of(n * CHUNK, CHUNK)
        rows = wt[pl.ds(first, CHUNK), :]
        z = dot_nn(rows, ht[0])
        for d in range(N_DEV):
            z_next = dot_nn(rows, ht[d + 1]) if d + 1 < N_DEV else None
            dz = grad_logits(z, stats, d, lab[d:d + 1, :], first)
            part = dot_nt(ht[d], dz)
            gw_buf[n] = part if d == 0 else gw_buf[n] + part
            z = z_next
        pair.start(c)

        @pl.when(c == 0)
        def _():
            da_relay.pass_on()
            dc_relay.pass_on()

        @pl.when(c == 1)
        def _():
            da_relay.pass_diagonal()
            dc_relay.pass_diagonal()

        @pl.when(c >= 2)
        def _():
            pair.pass_on(c - 2)

        return 0

    lax.fori_loop(0, 4, chunk, 0)
    da_relay.finish()
    dc_relay.finish()

    total = jnp.zeros((1, TILE), F32)
    for d in range(N_DEV):
        own = jnp.where(iota((1, TILE), 1) < OCT, stats[d, DIAGS:25, :], 0.0)
        total = total - (pltpu.roll(own, OCT * d, 1) if d else own)
    loss[...] = total[:, 0:HALF]

    def flip(x):
        width = x.shape[0]
        return jnp.concatenate([dot_nt(ident[:min(CHUNK, DIM - lo), :min(CHUNK, DIM - lo)], x[:, lo:lo + CHUNK]).astype(BF16)
                                for lo in range(0, DIM, CHUNK)], axis=0)

    for d in range(0, N_DEV, 2):
        fs = jnp.concatenate([f_all[d], f_all[d + 1]], axis=0)
        das = jnp.concatenate([da_all[d], da_all[d + 1]], axis=1)
        part = dot_nt(flip(fs), das)
        gw_enc[...] = part if d == 0 else gw_enc[...] + part
    for d in range(0, N_DEV, 4):
        dcs = jnp.concatenate([jnp.concatenate([dc_all[d + i, :, 0:HALF], dc_all[d + i, :, HALF:TILE]], axis=0)
                               for i in range(4)], axis=1).astype(BF16)
        part = dot_nt(flip(g[d * HALF:(d + 4) * HALF, :]), dcs)
        gw_pred[...] = part if d == 0 else gw_pred[...] + part
    pick = jnp.where(iota((16, TILE), 1) == iota((16, TILE), 0) + me * 16, 1.0, 0.0).astype(BF16)
    rows = jnp.concatenate([dot_nt(pick, da_all[d]).astype(BF16) for d in range(N_DEV)], axis=0)
    grad_enc[...] = dot_nt(rows, w_enc[...]).reshape(HALF, 2, DIM).astype(BF16)

    pair.pass_on(2)
    pair.pass_on(3)
    for c in range(4):
        pair.finish(c)
    for copy in copies:
        copy.wait_send()
    st_gather.wait_send()


def flush_kernel(loss, grad_enc, gw_enc, gw_pred, gw_buf, loss_out, grad_enc_out, gw_enc_out, gw_pred_out, gw_out, out_sem):
    moves = [(gw_buf.at[n], gw_out.at[:, n * CHUNK:(n + 1) * CHUNK]) for n in range(VOCAB // CHUNK)]
    moves += [(loss, loss_out), (grad_enc, grad_enc_out), (gw_enc, gw_enc_out), (gw_pred, gw_pred_out)]
    moves = [pltpu.make_async_copy(src, dst, out_sem.at[k]) for k, (src, dst) in enumerate(moves)]
    for copy in moves:
        copy.start()
    for copy in moves:
        copy.wait()


def vmem():
    return pl.BlockSpec(memory_space=pltpu.VMEM)


def solution(mesh):
    dma = pltpu.SemaphoreType.DMA

    def local_fn(enc_out, pred_out, w_enc, w_pred, w_out, labels, frame_len, label_len):
        n_utt = pred_out.shape[0]
        g = pred_out.reshape(OCT * n_utt, DIM)
        hbm = pl.BlockSpec(memory_space=pl.ANY)
        mem = pltpu.VMEM
        outs = [((1, n_utt), F32), (enc_out.shape, BF16), ((DIM, DIM), F32), ((DIM, DIM), F32)]
        handed = pl.pallas_call(
            main_kernel,
            out_shape=tuple(mem(shape, kind) for shape, kind in outs + [((16, DIM, CHUNK), F32)]),
            in_specs=[vmem()] + [hbm] * 4 + [vmem()] * 3,
            out_specs=(vmem(),) * 5,
            scratch_shapes=[mem((TILE, DIM), BF16), mem((512, DIM), BF16), mem((DIM, DIM), BF16), mem((DIM, VOCAB), BF16),
                            mem((VOCAB, DIM), BF16), mem((OCT, DIM, LANES), BF16), mem((VOCAB, LANES), F32),
                            mem((WIDE, LANES), BF16), mem((2, DIM, WIDE), BF16), mem((OCT, DIM, HALF), BF16), mem((DIM, DIM), BF16),
                            mem((OCT, DIM, TILE), BF16), mem((OCT, MID, TILE), F32), mem((OCT, TILE, DIM), BF16),
                            mem((OCT, 32, TILE), F32), mem((2, 40, TILE), F32), mem((OCT, TILE), jnp.int32),
                            mem((OCT, TILE), jnp.int32), mem((1, TILE), jnp.int32), dma((7,))]
            + [dma((OCT,))] * 4 + [dma((4, 5))] * 2 + [dma((9,))] * 6,
            compiler_params=pltpu.CompilerParams(collective_id=0, has_side_effects=True, vmem_limit_bytes=MAIN_VMEM),
        )(enc_out, g, w_enc, w_pred, w_out, labels.T, frame_len.reshape(1, n_utt), label_len.reshape(1, n_utt))
        outs.append(((DIM, VOCAB), F32))
        loss, grad_enc, gw_enc, gw_pred, gw_out = pl.pallas_call(
            flush_kernel,
            out_shape=tuple(jax.ShapeDtypeStruct(shape, kind) for shape, kind in outs),
            in_specs=[vmem()] * 5,
            out_specs=(hbm,) * 5,
            scratch_shapes=[dma((20,))],
            compiler_params=pltpu.CompilerParams(vmem_limit_bytes=LAST_VMEM),
        )(*handed)
        return loss.reshape(n_utt), grad_enc, gw_enc, gw_pred, gw_out

    in_specs = (P('dp', 'seq', None), P('dp', None, None), P(None, None), P(None, None), P(None, None), P('dp', None), P('dp'), P('dp'))
    out_specs = (P('dp'), P('dp', 'seq', None), P('dp', None), P('dp', None), P('dp', None))
    return jax.shard_map(local_fn, mesh=mesh, in_specs=in_specs, out_specs=out_specs, check_vma=False)
```

```python
import jax
import jax.numpy as jnp
from jax import lax
from jax.experimental import pallas as pl
from jax.experimental.pallas import tpu as pltpu
from jax.sharding import PartitionSpec as P

NEG = -1.0e30
F32 = jnp.float32
BF16 = jnp.bfloat16
N_DEV = 8
DIM = 640
VOCAB = 4096
LANES = 1024
CHUNK = 256
MAIN_VMEM = 53_000_000
LAST_VMEM = 1_000_000
OCT, DIAGS, HALF, TILE, WIDE, MID = 8, 24, 64, 128, 192, 320


def dot_nn(lhs, rhs):
    return lax.dot_general(lhs, rhs, (((1,), (0,)), ((), ())), preferred_element_type=F32)


def dot_nt(lhs, rhs):
    return lax.dot_general(lhs, rhs, (((1,), (1,)), ((), ())), preferred_element_type=F32)


def iota(shape, axis):
    return lax.broadcasted_iota(jnp.int32, shape, axis)


def eye(size):
    return jnp.where(iota((size, size), 0) == iota((size, size), 1), 1.0, 0.0).astype(BF16)


def transpose_into(dst, src, ident):
    cols = src.shape[1]
    for lo in range(0, cols, CHUNK):
        width = min(CHUNK, cols - lo)
        dst[lo:lo + width, :] = dot_nt(ident[:width, :width], src[:, lo:lo + width]).astype(BF16)


def logaddexp(a, b):
    top = jnp.maximum(a, b)
    return top + jnp.log(1.0 + jnp.exp(-jnp.abs(a - b)))


class Peers:
    def __init__(self):
        self.dp = lax.axis_index('dp')
        self.me = lax.axis_index('seq')
        core = lax.rem(self.me, 2)
        col = lax.rem(self.me // 2, 2)
        row = self.me // 4
        self.core = core
        self.diag = lax.rem(row + col, 2)
        self.pp = row * 4 + col * 2 + (1 - core)
        self.px = row * 4 + (1 - col) * 2 + core
        self.py = (1 - row) * 4 + col * 2 + core
        self.pd = (1 - row) * 4 + (1 - col) * 2 + core
        self.px_p = row * 4 + (1 - col) * 2 + (1 - core)
        self.py_p = (1 - row) * 4 + col * 2 + (1 - core)
        self.pd_p = (1 - row) * 4 + (1 - col) * 2 + (1 - core)

    def target(self, seq):
        return (self.dp, seq)


def remote(src, dst, send_sem, recv_sem, device):
    return pltpu.make_async_remote_copy(src_ref=src, dst_ref=dst, send_sem=send_sem, recv_sem=recv_sem,
                                        device_id=device, device_id_type=pl.DeviceIdType.MESH)


class Relay:
    def __init__(self, peers, view, half, send_sem, recv_sem):
        self.p = peers
        self.view = view
        self.half = half
        self.ssem = send_sem
        self.rsem = recv_sem

    def copy(self, kind, block, device):
        return remote(block, block, self.ssem.at[kind], self.rsem.at[kind], self.p.target(device))

    def stage(self, number, x, y, d):
        p = self.p
        if number == 0:
            base, pairs = 0, ((p.px, self.view(p.me)), (p.py, self.view(p.me)), (p.pp, self.view(x)))
        elif number == 1:
            base, pairs = 3, ((p.py, self.half(x, 0)), (p.px, self.half(y, 1)), (p.pp, self.view(x)), (p.pp, self.view(y)))
        else:
            base, pairs = 7, ((p.pp, self.half(d, 0)), (p.pp, self.half(d, 1)))
        return [self.copy(base + i, block, device) for i, (device, block) in enumerate(pairs)]

    def start(self):
        for copy in self.stage(0, self.p.me, None, None):
            copy.start()

    def pass_on(self):
        p = self.p
        from_x = self.copy(0, self.view(p.px), p.px)
        from_y = self.copy(1, self.view(p.py), p.py)
        to_y, to_x, x_over, y_over = self.stage(1, p.px, p.py, None)
        from_x.wait_recv()
        to_y.start()
        x_over.start()
        from_y.wait_recv()
        to_x.start()
        y_over.start()

    def pass_diagonal(self):
        p = self.p
        self.copy(3, self.half(p.pd, 0), p.py).wait_recv()
        self.copy(4, self.half(p.pd, 1), p.px).wait_recv()
        for copy in self.stage(2, None, None, p.pd):
            copy.start()

    def finish(self):
        p = self.p
        self.stage(0, p.pp, None, None)[2].wait_recv()
        for copy in self.stage(1, p.px_p, p.py_p, None)[2:] + self.stage(2, None, None, p.pd_p):
            copy.wait_recv()
        for copy in self.stage(0, p.me, None, None) + self.stage(1, p.px, p.py, None) + self.stage(2, None, None, p.pd):
            copy.wait_send()


class Pair:
    def __init__(self, peers, buf, mine, other, send_sem, recv_sem):
        self.p = peers
        self.buf = buf
        self.mine = mine
        self.other = other
        self.ssem = send_sem
        self.rsem = recv_sem

    def copy(self, c, kind, block, device):
        return remote(block, block, self.ssem.at[c, kind], self.rsem.at[c, kind], self.p.target(device))

    def half(self, base, core, c, h):
        return self.buf.at[(base + core) * 4 + c, h * MID:(h + 1) * MID, :]

    def start(self, c):
        p = self.p
        self.copy(c, 1, self.half(self.mine, p.core, c, 0), p.px).start()
        self.copy(c, 2, self.half(self.mine, p.core, c, 1), p.py).start()
        self.copy(c, 0, self.buf.at[(self.mine + p.core) * 4 + c], p.pp).start()

    def pass_on(self, c):
        p = self.p
        low = self.half(self.other, p.core, c, 0)
        high = self.half(self.other, p.core, c, 1)
        self.copy(c, 1, low, p.px).wait_recv()
        self.copy(c, 3, low, p.pp).start()
        self.copy(c, 2, high, p.py).wait_recv()
        self.copy(c, 4, high, p.pp).start()

    def finish(self, c):
        p = self.p
        twin = 1 - p.core
        self.copy(c, 0, self.buf.at[(self.mine + twin) * 4 + c], p.pp).wait_recv()
        self.copy(c, 3, self.half(self.other, twin, c, 0), p.pp).wait_recv()
        self.copy(c, 4, self.half(self.other, twin, c, 1), p.pp).wait_recv()
        self.copy(c, 0, self.buf.at[(self.mine + p.core) * 4 + c], p.pp).wait_send()
        self.copy(c, 1, self.half(self.mine, p.core, c, 0), p.px).wait_send()
        self.copy(c, 2, self.half(self.mine, p.core, c, 1), p.py).wait_send()
        self.copy(c, 3, self.half(self.other, p.core, c, 0), p.pp).wait_send()
        self.copy(c, 4, self.half(self.other, p.core, c, 1), p.pp).wait_send()


class Direct:
    def __init__(self, peers, src, dst, send_sem, recv_sem):
        self.p = peers
        self.src = src
        self.dst = dst
        self.ssem = send_sem
        self.rsem = recv_sem

    def copy(self, k, to, source):
        return remote(self.src(to), self.dst(source), self.ssem.at[k], self.rsem.at[k], self.p.target(to))

    def start(self):
        for k in range(1, N_DEV):
            self.copy(k, lax.rem(self.p.me + k, N_DEV), self.p.me).start()

    def wait_recv(self):
        for k in range(1, N_DEV):
            self.copy(k, lax.rem(self.p.me + k, N_DEV), lax.rem(self.p.me + N_DEV - k, N_DEV)).wait_recv()

    def wait_send(self):
        for k in range(1, N_DEV):
            self.copy(k, lax.rem(self.p.me + k, N_DEV), self.p.me).wait_send()


def pick_rows(ref, offsets, group):
    out = None
    for u, off in enumerate(offsets):
        part = ref[off:off + DIAGS, :]
        out = part if out is None else jnp.where(group == u, part, out)
    return out


def lattice(lse, z_blank, z_lab, n_frames, n_labels, me, skew, stats):
    lane = iota((1, TILE), 1)
    group = lax.rem(lane // OCT, OCT)

    def by_time(x):
        return jnp.concatenate([x, pltpu.roll(x, HALF, 1)], axis=0)

    skew[...] = jnp.zeros_like(skew)
    skew[0, OCT:DIAGS, :] = by_time(z_blank - lse)
    skew[1, OCT:DIAGS, :] = by_time(z_lab - lse)
    offsets = [OCT - u for u in range(OCT)]
    group24 = jnp.broadcast_to(group, (DIAGS, TILE))
    blank = pick_rows(skew.at[0], offsets, group24)
    lab = pick_rows(skew.at[1], offsets, group24)

    first_u = group == 0
    last_u = group == 7
    alpha = jnp.where(first_u, 0.0, NEG).astype(F32)
    alphas = [alpha]
    for d in range(1, 23):
        stay = alpha + blank[d - 1:d]
        step = jnp.where(first_u, NEG, pltpu.roll(alpha + lab[d - 1:d], OCT, 1))
        alpha = logaddexp(stay, step)
        alphas.append(alpha)
    alphas.append(jnp.full((1, TILE), NEG, F32))
    bound = jnp.where(group == n_labels, 0.0, NEG).astype(F32)
    beta = bound
    nexts, ups = [None] * DIAGS, [None] * DIAGS
    nexts[23] = ups[23] = jnp.full((1, TILE), NEG, F32)
    for d in range(22, -1, -1):
        up = jnp.where(last_u, NEG, pltpu.roll(beta, 120, 1))
        nexts[d], ups[d] = beta, up
        new = logaddexp(beta + blank[d:d + 1], up + lab[d:d + 1])
        beta = jnp.where(d - group >= n_frames, bound, new)
    log_p = jnp.where(lane < OCT, beta, 0.0)
    for shift in (OCT, 16, 32, HALF):
        log_p = log_p + pltpu.roll(log_p, shift, 1)

    alphas = jnp.concatenate(alphas, axis=0)
    nexts = jnp.concatenate(nexts, axis=0)
    ups = jnp.concatenate(ups, axis=0)
    frame = iota((DIAGS, TILE), 0) - group24
    ok = (frame >= 0) & (frame < n_frames)
    occ_b = jnp.where(ok, jnp.exp(jnp.minimum(alphas + blank + nexts - log_p, 0.0)), 0.0)
    occ_l = jnp.where(ok & (group24 < 7), jnp.exp(jnp.minimum(alphas + lab + ups - log_p, 0.0)), 0.0)
    skew[0, 0:DIAGS, :] = occ_b
    skew[1, 0:DIAGS, :] = occ_l
    offsets = list(range(OCT))
    low = jnp.broadcast_to(lane < HALF, (OCT, TILE))

    def by_tile(x):
        return jnp.where(low, x[0:OCT], pltpu.roll(x[OCT:16], HALF, 1))

    stats[me, 0:OCT, :] = lse
    stats[me, OCT:16, :] = by_tile(pick_rows(skew.at[0], offsets, group24))
    stats[me, 16:DIAGS, :] = by_tile(pick_rows(skew.at[1], offsets, group24))
    stats[me, DIAGS:32, :] = jnp.broadcast_to(log_p, (OCT, TILE))


def grad_logits(z, stats, block, lab, first_id, col0=0, has_blank=None):
    rows, cols = z.shape
    ids = iota((rows, TILE), 0) + first_id
    tiles = []
    for k in range(cols // TILE):
        kk = k + col0
        lse = stats[block, kk:kk + 1, :]
        occ_b = stats[block, OCT + kk:9 + kk, :]
        occ_l = stats[block, 16 + kk:17 + kk, :]
        tile = jnp.exp(z[:, k * TILE:(k + 1) * TILE] - lse) * (occ_b + occ_l)
        tile = tile - jnp.where(ids == lab, occ_l, 0.0)
        head = tile[0:16] - jnp.where(ids[0:16] == 0, occ_b, 0.0)
        tiles.append(jnp.concatenate([head, tile[16:]], axis=0).astype(BF16))
    return jnp.concatenate(tiles, axis=1)


def own_lengths(ref, scratch, me):
    scratch[...] = jnp.zeros_like(scratch)
    scratch[:, 0:HALF] = ref[...]
    x = pltpu.roll(scratch[...], lax.rem(TILE - OCT * me, TILE), 1)
    x = jnp.where(iota((1, TILE), 1) < OCT, x, 0)
    for shift in (OCT, 16, 32, HALF):
        x = x + pltpu.roll(x, shift, 1)
    return x


def spread_labels(labels, scratch, lab):
    scratch[...] = jnp.full_like(scratch, -1)
    scratch[0:7, 0:HALF] = labels[...]
    scratch[0:7, HALF:TILE] = labels[...]
    x = pltpu.roll(scratch[...], 0, 1, stride=OCT, stride_axis=0)
    keep = lax.rem(iota((OCT, TILE), 1) // OCT, OCT) == iota((OCT, TILE), 0)
    for d in range(N_DEV):
        turned = pltpu.roll(x, TILE - OCT * d, 1) if d else x
        lab[d:d + 1, :] = jnp.sum(jnp.where(keep, turned, 0), axis=0, keepdims=True)


def main_kernel(enc3, g_hbm, we_hbm, wp_hbm, w_hbm, labels, frame_len, label_len,
                loss, grad_enc, gw_enc, gw_pred, gw_buf,
                enc, g, w_out, wt, ht, zs, sel, act, c_all, wet, da_all, dc_all, f_all, stats, skew, lab, lab_x, len_x,
                load_sem, a2a_s, a2a_r, st_s, st_r, gw_s, gw_r, f_s, f_r, da_s, da_r, dc_s, dc_r):
    p = Peers()
    me = p.me
    barrier = pltpu.get_barrier_semaphore()
    for k in range(1, N_DEV):
        pl.semaphore_signal(barrier, inc=1, device_id=p.target(lax.rem(me + k, N_DEV)),
                            device_id_type=pl.DeviceIdType.MESH)
    w_pred, wpt, w_enc = ht.at[0, :, 0:DIM], ht.at[1, :, 0:DIM], ht.at[2, :, 0:DIM]
    loads = [(wp_hbm, w_pred), (g_hbm, g), (we_hbm, w_enc)]
    for lo in range(0, VOCAB, LANES):
        loads.append((w_hbm.at[:, lo:lo + LANES], w_out.at[:, lo:lo + LANES]))
    loads = [pltpu.make_async_copy(src, dst, load_sem.at[k]) for k, (src, dst) in enumerate(loads)]
    for copy in loads:
        copy.start()
    enc[...] = enc3[...].reshape(TILE, DIM)
    pl.semaphore_wait(barrier, N_DEV - 1)

    def rows16(i):
        return pl.ds(pl.multiple_of(i * 16, 16), 16)

    copies = []
    for k in range(1, N_DEV):
        to = lax.rem(me + k, N_DEV)
        copies.append(remote(enc.at[rows16(to), :], f_all.at[to, rows16(me), :], a2a_s.at[k], a2a_r.at[k], p.target(to)))
    for copy in copies:
        copy.start()
    f_all[me, rows16(me), :] = enc[rows16(me), :]

    ident = eye(CHUNK)
    row = iota((WIDE, LANES), 0)
    col = iota((WIDE, LANES), 1)
    t_id = col // TILE + OCT * (lax.rem(col, TILE) // HALF)
    u_id = lax.rem(col // OCT, OCT)
    b_id = lax.rem(col, OCT)
    a_row = 2 * (row // 16) + lax.rem(row, 2)
    a_b = lax.rem(row // 2, OCT)
    c_row = row - TILE
    hit = jnp.where(row < TILE, jnp.where((a_row == t_id) & (a_b == b_id), 1.0, 0.0),
                    jnp.where((c_row // OCT == b_id) & (lax.rem(c_row, OCT) == u_id), 1.0, 0.0))
    sel[...] = hit.astype(BF16)
    spread_labels(labels, lab_x, lab)
    n_frames = own_lengths(frame_len, len_x, me)
    n_labels = own_lengths(label_len, len_x, me)
    first_loads, last_loads = loads[:3], loads[3:]
    for copy in first_loads:
        copy.wait()
    transpose_into(wpt, w_pred, ident)
    transpose_into(wet, w_enc, ident)
    c_cols = dot_nt(wpt[...], g[...]).astype(BF16)
    for k in range(4):
        c_all[k] = c_cols[:, k * TILE:(k + 1) * TILE]

    def transpose_out(c, _):
        lo = pl.multiple_of(c * CHUNK, CHUNK)
        wt[pl.ds(lo, CHUNK), :] = dot_nt(ident, w_out[:, pl.ds(lo, CHUNK)]).astype(BF16)
        return 0

    for k, copy in enumerate(last_loads):
        copy.wait()
        lax.fori_loop(4 * k, 4 * k + 4, transpose_out, 0, unroll=4)

    for k in range(1, N_DEV):
        src = lax.rem(me + N_DEV - k, N_DEV)
        remote(enc.at[rows16(me), :], f_all.at[me, rows16(src), :], a2a_s.at[k], a2a_r.at[k], p.target(src)).wait_recv()

    f_relay = Relay(p, lambda e: f_all.at[e], lambda e, h: f_all.at[e, h * HALF:(h + 1) * HALF, :], f_s, f_r)
    f_relay.start()

    def hidden(d, slot):
        act[slot, :, 0:TILE] = dot_nt(wet[...], f_all[d]).astype(BF16)
        two = c_all[d // 2]
        act[slot, :, TILE:WIDE] = jnp.where(lax.rem(d, 2) == 1, two[:, HALF:TILE], two[:, 0:HALF])
        ht[d] = jnp.tanh(dot_nn(act[slot], sel[...])).astype(BF16)

    hidden(me, 0)
    lab_own = lab[pl.ds(me, 1), :]
    lab_row = jnp.concatenate([lab_own] * OCT, axis=1)

    def forward(c, carry):
        top, total, z_lab = carry
        lo = pl.multiple_of(c * CHUNK, CHUNK)
        z = dot_nn(wt[pl.ds(lo, CHUNK), :], ht[me])
        zs[pl.ds(lo, CHUNK), :] = z
        z = z.reshape(CHUNK // OCT, OCT, LANES)
        new = jnp.maximum(top, jnp.max(z, axis=0))
        total = total * jnp.exp(top - new) + jnp.sum(jnp.exp(z - new[None]), axis=0)
        ids = iota(z.shape, 0) * OCT + iota(z.shape, 1) + lo
        z_lab = z_lab + jnp.sum(jnp.where(ids == lab_row[None], z, 0.0), axis=0)
        return new, total, z_lab

    carry = (jnp.full((OCT, LANES), NEG, F32), jnp.zeros((OCT, LANES), F32), jnp.zeros((OCT, LANES), F32))
    carry = lax.fori_loop(0, OCT, forward, carry, unroll=8)
    f_relay.pass_on()
    top, total, z_lab = lax.fori_loop(OCT, 16, forward, carry, unroll=8)
    f_relay.pass_diagonal()
    peak = jnp.max(top, axis=0, keepdims=True)
    lse = peak + jnp.log(jnp.sum(total * jnp.exp(top - peak), axis=0, keepdims=True))
    z_lab = jnp.sum(z_lab, axis=0, keepdims=True)
    z_blank = zs[0:1, :]

    def tiles(x):
        return jnp.concatenate([x[:, k * TILE:(k + 1) * TILE] for k in range(OCT)], axis=0)

    lattice(tiles(lse), tiles(z_blank), tiles(z_lab), n_frames, n_labels, me, skew, stats)
    st_gather = Direct(p, lambda d: stats.at[me], lambda i: stats.at[i], st_s, st_r)
    st_gather.start()

    f_relay.finish()
    for k in range(1, N_DEV):
        hidden(lax.rem(me + k, N_DEV), k % 2)

    mine = 2 * p.diag
    own_set = mine + p.core
    slots = [own_set * 4 + j for j in range(4)]
    for slot in slots:
        gw_buf[slot] = jnp.zeros((DIM, CHUNK), F32)

    def backward(i, _):
        lo = pl.multiple_of(i * 512, 512)
        dz = grad_logits(zs[pl.ds(lo, 512), :], stats, me, lab_own, lo)
        part = dot_nn(w_out[:, pl.ds(lo, 512)], dz)
        for j, slot in enumerate(slots):
            gw_buf[slot] += part[:, j * CHUNK:(j + 1) * CHUNK]
        return 0

    lax.fori_loop(0, OCT, backward, 0, unroll=4)
    sums = None
    for j, slot in enumerate(slots):
        cols = slice(j * CHUNK, (j + 1) * CHUNK)
        h32 = ht[me, :, cols].astype(F32)
        dp = (gw_buf[slot] * (1.0 - h32 * h32)).astype(BF16)
        part = dot_nt(dp, sel[:, cols])
        sums = part if sums is None else sums + part
    da_all[me] = sums[:, 0:TILE].astype(BF16)
    dc_all[me] = jnp.concatenate([sums[0:MID, TILE:WIDE], sums[MID:DIM, TILE:WIDE]], axis=1)
    da_relay = Relay(p, lambda e: da_all.at[e], lambda e, h: da_all.at[e, h * MID:(h + 1) * MID, :], da_s, da_r)
    dc_relay = Relay(p, lambda e: dc_all.at[e], lambda e, h: dc_all.at[e, h * 160:(h + 1) * 160, :], dc_s, dc_r)
    da_relay.start()
    dc_relay.start()

    st_gather.wait_recv()
    pair = Pair(p, gw_buf, mine, 2 - mine, gw_s, gw_r)

    def chunk(c, _):
        n = own_set * 4 + c
        first = pl.multiple_of(n * CHUNK, CHUNK)
        rows = wt[pl.ds(first, CHUNK), :]
        z = dot_nn(rows, ht[0])
        for d in range(N_DEV):
            z_next = dot_nn(rows, ht[d + 1]) if d + 1 < N_DEV else None
            dz = grad_logits(z, stats, d, lab[d:d + 1, :], first)
            part = dot_nt(ht[d], dz)
            gw_buf[n] = part if d == 0 else gw_buf[n] + part
            z = z_next
        pair.start(c)

        @pl.when(c == 1)
        def _():
            da_relay.pass_on()
            dc_relay.pass_on()

        @pl.when(c == 2)
        def _():
            da_relay.pass_diagonal()
            dc_relay.pass_diagonal()

        @pl.when(c >= 2)
        def _():
            pair.pass_on(c - 2)

        return 0

    lax.fori_loop(0, 4, chunk, 0)
    da_relay.finish()
    dc_relay.finish()

    total = jnp.zeros((1, TILE), F32)
    for d in range(N_DEV):
        own = jnp.where(iota((1, TILE), 1) < OCT, stats[d, DIAGS:25, :], 0.0)
        total = total - (pltpu.roll(own, OCT * d, 1) if d else own)
    loss[...] = total[:, 0:HALF]

    def flip(x):
        width = x.shape[0]
        return jnp.concatenate([dot_nt(ident[:min(CHUNK, DIM - lo), :min(CHUNK, DIM - lo)], x[:, lo:lo + CHUNK]).astype(BF16)
                                for lo in range(0, DIM, CHUNK)], axis=0)

    for d in range(0, N_DEV, 2):
        fs = jnp.concatenate([f_all[d], f_all[d + 1]], axis=0)
        das = jnp.concatenate([da_all[d], da_all[d + 1]], axis=1)
        part = dot_nt(flip(fs), das)
        gw_enc[...] = part if d == 0 else gw_enc[...] + part
    for d in range(0, N_DEV, 4):
        dcs = jnp.concatenate([jnp.concatenate([dc_all[d + i, :, 0:HALF], dc_all[d + i, :, HALF:TILE]], axis=0)
                               for i in range(4)], axis=1).astype(BF16)
        part = dot_nt(flip(g[d * HALF:(d + 4) * HALF, :]), dcs)
        gw_pred[...] = part if d == 0 else gw_pred[...] + part
    pick = jnp.where(iota((16, TILE), 1) == iota((16, TILE), 0) + me * 16, 1.0, 0.0).astype(BF16)
    rows = jnp.concatenate([dot_nt(pick, da_all[d]).astype(BF16) for d in range(N_DEV)], axis=0)
    grad_enc[...] = dot_nn(rows, wet[...]).reshape(HALF, 2, DIM).astype(BF16)

    pair.pass_on(2)
    pair.pass_on(3)
    for c in range(4):
        pair.finish(c)
    for copy in copies:
        copy.wait_send()
    st_gather.wait_send()


def flush_kernel(loss, grad_enc, gw_enc, gw_pred, gw_buf, loss_out, grad_enc_out, gw_enc_out, gw_pred_out, gw_out, out_sem):
    moves = [(gw_buf.at[n], gw_out.at[:, n * CHUNK:(n + 1) * CHUNK]) for n in range(VOCAB // CHUNK)]
    moves += [(loss, loss_out), (grad_enc, grad_enc_out), (gw_enc, gw_enc_out), (gw_pred, gw_pred_out)]
    moves = [pltpu.make_async_copy(src, dst, out_sem.at[k]) for k, (src, dst) in enumerate(moves)]
    for copy in moves:
        copy.start()
    for copy in moves:
        copy.wait()


def vmem():
    return pl.BlockSpec(memory_space=pltpu.VMEM)


def solution(mesh):
    dma = pltpu.SemaphoreType.DMA

    def local_fn(enc_out, pred_out, w_enc, w_pred, w_out, labels, frame_len, label_len):
        n_utt = pred_out.shape[0]
        g = pred_out.reshape(OCT * n_utt, DIM)
        hbm = pl.BlockSpec(memory_space=pl.ANY)
        mem = pltpu.VMEM
        outs = [((1, n_utt), F32), (enc_out.shape, BF16), ((DIM, DIM), F32), ((DIM, DIM), F32)]
        handed = pl.pallas_call(
            main_kernel,
            out_shape=tuple(mem(shape, kind) for shape, kind in outs + [((16, DIM, CHUNK), F32)]),
            in_specs=[vmem()] + [hbm] * 4 + [vmem()] * 3,
            out_specs=(vmem(),) * 5,
            scratch_shapes=[mem((TILE, DIM), BF16), mem((512, DIM), BF16), mem((DIM, VOCAB), BF16),
                            mem((VOCAB, DIM), BF16), mem((OCT, DIM, LANES), BF16), mem((VOCAB, LANES), F32),
                            mem((WIDE, LANES), BF16), mem((2, DIM, WIDE), BF16), mem((4, DIM, TILE), BF16), mem((DIM, DIM), BF16),
                            mem((OCT, DIM, TILE), BF16), mem((OCT, MID, TILE), F32), mem((OCT, TILE, DIM), BF16),
                            mem((OCT, 32, TILE), F32), mem((2, 40, TILE), F32), mem((OCT, TILE), jnp.int32),
                            mem((OCT, TILE), jnp.int32), mem((1, TILE), jnp.int32), dma((7,))]
            + [dma((OCT,))] * 4 + [dma((4, 5))] * 2 + [dma((9,))] * 6,
            compiler_params=pltpu.CompilerParams(collective_id=0, has_side_effects=True, vmem_limit_bytes=MAIN_VMEM),
        )(enc_out, g, w_enc, w_pred, w_out, labels.T, frame_len.reshape(1, n_utt), label_len.reshape(1, n_utt))
        outs.append(((DIM, VOCAB), F32))
        loss, grad_enc, gw_enc, gw_pred, gw_out = pl.pallas_call(
            flush_kernel,
            out_shape=tuple(jax.ShapeDtypeStruct(shape, kind) for shape, kind in outs),
            in_specs=[vmem()] * 5,
            out_specs=(hbm,) * 5,
            scratch_shapes=[dma((20,))],
            compiler_params=pltpu.CompilerParams(vmem_limit_bytes=LAST_VMEM),
        )(*handed)
        return loss.reshape(n_utt), grad_enc, gw_enc, gw_pred, gw_out

    in_specs = (P('dp', 'seq', None), P('dp', None, None), P(None, None), P(None, None), P(None, None), P('dp', None), P('dp'), P('dp'))
    out_specs = (P('dp'), P('dp', 'seq', None), P('dp', None), P('dp', None), P('dp', None))
    return jax.shard_map(local_fn, mesh=mesh, in_specs=in_specs, out_specs=out_specs, check_vma=False)
```
